32 devices in a mesh: img: 8 (over y, x, core), cls: 4 (over z).
Axes of the slice: x: 2, y: 2, z: 4, core: 2. Of those that a mesh axis runs over, the one named last changes fastest.
Arguments:
- images: bfloat16 [64, 9216], P('img'), may hold values from -64 to 64
- references: bfloat16 [512, 9216], P(('img', 'cls')), may hold values from -0.2 to 0.2
- class_logprior: bfloat16 [512], P(('img', 'cls')), may hold values from -3 to 3
- ctf_table: float32 [16, 32], replicated, may hold values from -1 to 1, as said below
- noise_power: float32 [32], replicated, may hold values from 0.5 to 2
- tau_power: float32 [32], replicated, may hold values from 0.5 to 4
- defocus: int32 [64], P('img'), may hold values from 0 to 15
- offsets: int32 [64, 4, 2], P('img'), may hold values from -3 to 3
Outputs:
- new_refs: float32 [512, 9216], P(('img', 'cls'))
- new_weights: float32 [512], P(('img', 'cls'))
- loglik: float32 [64], P('img')
The draws below stay inside these ranges and needn't reach their ends.
Inputs may be any that keep to these rules, and one draw needn't show every extreme that they name: `ctf_table`: each row is a contrast transfer curve that oscillates over the cycles.
All inputs are finite; a program needn't handle non-finite values.
Results may differ from the reference program's by a relative error of at most 0.0068.
Values may be sent and summed in bfloat16 or wider, within the bound.
A program may use at most 64 MiB of HBM per device.

```python
import math
import jax
import jax.numpy as jnp
from jax import lax

TRANS = 4
CYCLES = 32
ANG = 144
ROT = 36
K = 512
NDEF = 16
IMGS = 64


def draw_common(key):
    width = 2 * CYCLES * ANG
    keys = [jax.random.fold_in(key, 101 + number) for number in range(11)]
    refs = jnp.clip(jax.random.normal(keys[1], (K, width)) * 0.03, -0.2, 0.2)
    slope = jax.random.uniform(keys[2], (NDEF, 1), minval=0.002, maxval=0.02)
    radius = jnp.arange(CYCLES, dtype=jnp.float32) + 1.0
    curves = -jnp.sin(slope * radius[None, :] * radius[None, :] + 0.1)
    noise = jnp.exp(jax.random.uniform(keys[3], (CYCLES,), minval=math.log(0.5), maxval=math.log(2.0)))
    groups = jax.random.randint(keys[4], (IMGS,), 0, NDEF)
    shifts = jax.random.randint(keys[5], (IMGS, TRANS, 2), -3, 4)
    pictures = jnp.clip(jax.random.normal(keys[6], (IMGS, width)), -6.0, 6.0)
    return (refs, curves, noise, groups, shifts, pictures)


def draw_images(key, part):
    return draw_common(key)[5].astype(jnp.bfloat16)


def draw_references(key, part):
    return draw_common(key)[0].astype(jnp.bfloat16)


def draw_ctf_table(key, part):
    return draw_common(key)[1].astype(jnp.float32)


def draw_noise_power(key, part):
    return draw_common(key)[2].astype(jnp.float32)


def draw_defocus(key, part):
    return draw_common(key)[3].astype(jnp.int32)


def draw_offsets(key, part):
    return draw_common(key)[4].astype(jnp.int32)


def block_scale(own_key, shape, cuts, least, top_value):
    def one(dim, blocks):
        draws = jax.random.uniform(jax.random.fold_in(jax.random.fold_in(own_key, 6), dim), (blocks,), jnp.float32, least / len(cuts), top_value / len(cuts))
        return jnp.repeat(jnp.exp(draws), shape[dim] // blocks).reshape((-1,) + (1,) * (len(shape) - dim - 1))

    level = one(*cuts[0])
    for cut in cuts[1:]:
        level = level * one(*cut)
    return level


def gaussian(own_key, dims, scale, limit, pieces=(), kind=jnp.bfloat16):
    entries = scale * jax.random.normal(own_key, dims, jnp.float32)
    if pieces:
        entries = entries * block_scale(own_key, dims, pieces, -0.22, 0.18)
    return jnp.clip(entries, -limit, limit).astype(kind)


def setup_inputs(seed: int = 0) -> dict:
    splits = jax.random.split(jax.random.key(seed), 9)
    images = draw_images(jax.random.fold_in(splits[8], 71), 0)
    references = draw_references(jax.random.fold_in(splits[8], 71), 0)
    class_logprior = gaussian(splits[2], (K,), 0.5, 3.0, ((0, 32),))
    ctf_table = draw_ctf_table(jax.random.fold_in(splits[8], 71), 0)
    noise_power = draw_noise_power(jax.random.fold_in(splits[8], 71), 0)
    tau_power = jnp.clip(jnp.exp(jax.random.uniform(splits[5], (CYCLES,), jnp.float32, math.log(0.5), math.log(4.0))), 0.5, 4.0)
    defocus = draw_defocus(jax.random.fold_in(splits[8], 71), 0)
    offsets = draw_offsets(jax.random.fold_in(splits[8], 71), 0)
    return {"images": images, "references": references, "class_logprior": class_logprior, "ctf_table": ctf_table, "noise_power": noise_power, "tau_power": tau_power, "defocus": defocus, "offsets": offsets}


offset_sigma = 2.0


def phase_table(shift_x, shift_y):
    radius = jnp.arange(CYCLES, dtype=jnp.float32) + 1.0
    theta = 2.0 * math.pi * jnp.arange(ANG, dtype=jnp.float32) / ANG
    freq_x = radius[:, None] * jnp.cos(theta)[None, :]
    freq_y = radius[:, None] * jnp.sin(theta)[None, :]
    return -2.0 * math.pi * (shift_x[..., None, None] * freq_x + shift_y[..., None, None] * freq_y) / (2.0 * CYCLES)


def reference(images, references, class_logprior, ctf_table, noise_power, tau_power, defocus, offsets):
    width = 2 * CYCLES * ANG
    stride = ANG // ROT
    rows = IMGS * TRANS
    pixels = images.astype(jnp.float32).reshape(IMGS, 2, CYCLES, ANG)
    shift = offsets.astype(jnp.float32)
    angle = phase_table(shift[..., 0], shift[..., 1])
    cosine = jnp.cos(angle)
    sine = jnp.sin(angle)
    real_part = pixels[:, None, 0] * cosine - pixels[:, None, 1] * sine
    imag_part = pixels[:, None, 0] * sine + pixels[:, None, 1] * cosine
    shifted = jnp.stack([real_part, imag_part], axis=2)
    contrast = ctf_table[defocus]
    weighted = (shifted * (contrast / noise_power[None, :])[:, None, None, :, None]).astype(jnp.bfloat16).reshape(rows, width)
    inserted = (shifted * contrast[:, None, None, :, None]).astype(jnp.bfloat16).reshape(rows, width)
    norm_coef = contrast * contrast / (2.0 * noise_power[None, :])
    power = jnp.sum(jnp.square(references.astype(jnp.float32).reshape(K, 2, CYCLES, ANG)), axis=(1, 3))
    penalty = jnp.dot(norm_coef, power.T, precision=lax.Precision.HIGHEST)
    trans_prior = -(shift[..., 0] * shift[..., 0] + shift[..., 1] * shift[..., 1]) / (2.0 * offset_sigma * offset_sigma)

    def score_block(chosen):
        shaped = chosen.reshape(8, 2, CYCLES, ANG)
        rotated = jnp.stack([jnp.roll(shaped, stride * turn, axis=-1) for turn in range(ROT)], axis=1).reshape(8 * ROT, width)
        return lax.dot_general(weighted, rotated, (((1,), (1,)), ((), ())), preferred_element_type=jnp.float32)

    cross = lax.map(score_block, references.reshape(K // 8, 8, width))
    cross = cross.reshape(K // 8, rows, 8, ROT).transpose(1, 0, 2, 3).reshape(IMGS, TRANS, K, ROT)
    logp = cross - penalty[:, None, :, None] + class_logprior.astype(jnp.float32)[None, None, :, None]
    logp = logp + trans_prior[:, :, None, None]
    per_image = logp.reshape(IMGS, TRANS * K * ROT)
    peak = jnp.max(per_image, axis=1)
    total = jnp.sum(jnp.exp(per_image - peak[:, None]), axis=1)
    loglik = peak + jnp.log(total)
    posterior = (jnp.exp(per_image - peak[:, None]) / total[:, None]).astype(jnp.bfloat16).reshape(rows, K, ROT)

    def insert_block(section):
        product = lax.dot_general(section, inserted, (((0,), (0,)), ((), ())), preferred_element_type=jnp.float32)
        product = product.reshape(8, ROT, 2, CYCLES, ANG)
        collected = jnp.zeros((8, 2, CYCLES, ANG), jnp.float32)
        for turn in range(ROT):
            collected = collected + jnp.roll(product[:, turn], -stride * turn, axis=-1)
        return collected

    sections = posterior.reshape(rows, K // 8, 8 * ROT).transpose(1, 0, 2)
    numer = lax.map(insert_block, sections).reshape(K, 2, CYCLES, ANG)
    post_sum = jnp.sum(posterior.astype(jnp.float32), axis=2)
    squared_rows = jnp.repeat(contrast * contrast, TRANS, axis=0)
    denom = lax.dot_general(post_sum, squared_rows, (((0,), (0,)), ((), ())), precision=lax.Precision.HIGHEST)
    weight = jnp.sum(post_sum, axis=0)
    fresh = numer / (denom[:, None, :, None] + 1.0 / tau_power[None, None, :, None])
    return fresh.reshape(K, width), weight / IMGS, loglik
```

```python
import math

import jax
import jax.numpy as jnp
import numpy as np
from jax import lax
from jax.experimental import pallas as pl
from jax.experimental.pallas import tpu as pltpu
from jax.sharding import PartitionSpec as P

TRANS = 4
CYCLES = 32
ANG = 144
ROT = 36
NDEF = 16

STRIDE = ANG // ROT
REACH = 3
SIDE = 2 * REACH + 1
COMBOS = SIDE * SIDE
TABLE_ROWS = 112
HIGH = lax.Precision.HIGHEST
offset_sigma = 2.0

LANE = 128
LOW = 8
GROUPS = CYCLES // LOW
SPAN = LOW * ANG
COLS = SPAN // LANE
MIX = ROT // COLS
TURN = LANE // MIX
SEG = LANE // LOW
TILES = GROUPS * COLS
WIDE = 2 * LANE
BY_LANE = (((1,), (1,)), ((), ()))
F32 = jnp.float32
BF16 = jnp.bfloat16


def phase_rows():
    group = np.arange(GROUPS)[:, None, None]
    column = np.arange(COLS)[None, :, None]
    lane = np.arange(LANE)[None, None, :]
    radius = group * LOW + lane % LOW + 1.0
    theta = 2.0 * math.pi * (column * SEG + lane // LOW) / ANG
    freq_x = (radius * np.cos(theta)).reshape(TILES, 1, LANE)
    freq_y = (radius * np.sin(theta)).reshape(TILES, 1, LANE)
    combo = np.arange(COMBOS)[None, :, None]
    dx = combo // SIDE - REACH
    dy = combo % SIDE - REACH
    angle = -2.0 * math.pi * (dx * freq_x + dy * freq_y) / (2.0 * CYCLES)
    full = np.concatenate([np.cos(angle), np.sin(angle)], axis=2)
    high = full.astype(jnp.bfloat16)
    low = (full - high.astype(np.float64)).astype(jnp.bfloat16)
    table = np.zeros((TILES, TABLE_ROWS, WIDE), jnp.bfloat16)
    table[:, :COMBOS] = high
    table[:, COMBOS : 2 * COMBOS] = low
    return table


def iota(shape, dim):
    return lax.broadcasted_iota(jnp.int32, shape, dim)


def onehot(mask):
    return jnp.where(mask, 1.0, 0.0).astype(F32)


def column_of(row, size):
    square = jnp.broadcast_to(row, (size, size))
    return jnp.sum(
        jnp.where(iota((size, size), 0) == iota((size, size), 1), square, 0.0), axis=1, keepdims=True
    )


def pick_segments(sources, seg):
    value = sources[0]
    for s in range(1, LOW):
        value = jnp.where(seg == s, sources[s], value)
    return value


def natural_to_mixed(block, j, seg):
    sources = []
    for s in range(LOW):
        cycle = (s - j) % LOW
        n = (cycle * COLS + j - s) // LOW
        sources.append(block(n))
    return pick_segments(sources, seg)


def kernel(
    n, m,
    images_hbm, refs_hbm, prior_ref, ctf_ref, noise_ref, tau_ref, defocus_ref, offsets_ref, table_hbm,
    fresh_ref, weight_ref, loglik_ref,
    images_nat, refs_nat, table, own, every, spin, blend, unblend, turned, weighted_a, weighted_b, inserted,
    acc, post, mixed, stat, stats,
    load_sem, left_sem, direct_sem, relay_left, relay_sem, cls_left, cls_sem, img_left, img_sem, keep_sem,
):
    local = images_nat.shape[0]
    owned = refs_nat.shape[0]
    count = n * local
    rows = count * TRANS
    width = stat.shape[1]
    height = ROT * owned
    step = MIX * owned
    weighted = (weighted_a, weighted_b)

    row_id, column_id = lax.axis_index("img"), lax.axis_index("cls")
    partner = row_id + 1 - 2 * lax.rem(row_id, 2)
    peers = [lax.rem(row_id + 2 * hop, n) for hop in range(1, n // 2)]
    above = [{"cls": lax.rem(column_id + hop, m)} for hop in range(1, m)]
    beside = [{"img": lax.rem(row_id + hop, n)} for hop in range(1, n)]

    loads = [
        pltpu.make_async_copy(images_hbm, images_nat, load_sem.at[0]),
        pltpu.make_async_copy(refs_hbm, refs_nat, load_sem.at[1]),
        pltpu.make_async_copy(table_hbm, table, load_sem.at[2]),
    ]
    for copy in loads:
        copy.start()
    barrier = pltpu.get_barrier_semaphore()
    for peer in above + beside:
        pl.semaphore_signal(barrier, inc=1, device_id=peer, device_id_type=pl.DeviceIdType.MESH)

    def send(src, dst, peer, left, landed):
        copy = pltpu.make_async_remote_copy(
            src_ref=src, dst_ref=dst, send_sem=left, recv_sem=landed,
            device_id=peer, device_id_type=pl.DeviceIdType.MESH,
        )
        copy.start()
        return copy

    source = iota((LANE, LANE), 0)
    target = iota((LANE, LANE), 1)
    for j in range(LOW):
        place = (source % SEG) * LOW + (source // SEG + (LOW - j)) % LOW
        blend[j] = onehot(target == place).astype(BF16)
        place = (target % SEG) * LOW + (target // SEG + (LOW - j)) % LOW
        back = onehot(source == place).astype(BF16)
        unblend[j, :LANE] = back
        unblend[j, LANE:] = back

    meta = jnp.zeros((local, WIDE), F32)
    lane = iota((local, WIDE), 1)
    meta = jnp.where(lane == 0, column_of(defocus_ref[...].astype(F32), local), meta)
    for t in range(TRANS):
        for axis in range(2):
            value = column_of(offsets_ref[t, axis : axis + 1].astype(F32), local)
            meta = jnp.where(lane == 1 + t + axis * TRANS, value, meta)
    own[0] = meta.astype(BF16)

    def mix(nat, size, j):
        seg = iota((size, LANE), 1) // SEG
        parts = []
        for g in range(GROUPS):
            for p in range(2):
                start = p * CYCLES * ANG + g * SPAN

                def block(k, start=start):
                    return nat[:, start + k * LANE : start + (k + 1) * LANE].astype(F32)

                parts.append(natural_to_mixed(block, j, seg))
        stacked = jnp.concatenate(parts, axis=0).astype(BF16)
        return jnp.dot(stacked, blend[j % LOW], preferred_element_type=F32)

    loads[0].wait()
    for j in range(COLS):
        moved = mix(images_nat, local, j).astype(BF16)
        for g in range(GROUPS):
            for p in range(2):
                index = g * 2 + p
                own[1 + g * COLS + j, :, p * LANE : (p + 1) * LANE] = moved[
                    index * local : (index + 1) * local
                ]

    pl.semaphore_wait(barrier, n + m - 2)

    def part_of(g):
        return pl.ds(0, COLS + 1) if g == 0 else pl.ds(1 + g * COLS, COLS)

    direct = [[None] * len(peers) for _ in range(GROUPS)]
    relays = [[None] * (len(peers) + 1) for _ in range(GROUPS)]
    for g in range(GROUPS):
        piece = part_of(g)
        for hop, peer in enumerate(peers):
            direct[g][hop] = send(
                own.at[piece], every.at[row_id, piece], {"img": peer}, left_sem.at[g, hop], direct_sem.at[g, hop]
            )
        relays[g][0] = send(
            own.at[piece], every.at[row_id, piece], {"img": partner}, relay_left.at[g, 0], relay_sem.at[g, 0]
        )
    keep = pltpu.make_async_copy(own, every.at[row_id], keep_sem.at[0])
    keep.start()

    loads[1].wait()
    for j in range(COLS):
        spin[j] = mix(refs_nat, owned, j)
    lane = iota((2 * GROUPS * owned, LANE), 1)
    for q in range(MIX):
        before = pltpu.roll(spin[COLS - 1], q * TURN, 1) if q else None
        for j in range(COLS):
            if q:
                here = pltpu.roll(spin[j], q * TURN, 1)
                value = jnp.where(lane < q * TURN, before, here).astype(BF16)
                before = here
            else:
                value = spin[j].astype(BF16)
            for g in range(GROUPS):
                for p in range(2):
                    index = g * 2 + p
                    for spot in ((COLS - j) % COLS, (COLS - j) % COLS + COLS):
                        turned[
                            g, spot * step + q * owned : spot * step + (q + 1) * owned, p * LANE : (p + 1) * LANE
                        ] = value[index * owned : (index + 1) * owned]
    power = [jnp.zeros((owned, LANE), F32) for _ in range(GROUPS)]
    for j in range(COLS):
        for g in range(GROUPS):
            for p in range(2):
                index = g * 2 + p
                entry = spin[j, index * owned : (index + 1) * owned]
                power[g] = power[g] + entry * entry
    power = jnp.concatenate(power, axis=1)
    spread = onehot(
        iota((CYCLES, GROUPS * LANE), 0)
        == iota((CYCLES, GROUPS * LANE), 1) // LANE * LOW + iota((CYCLES, GROUPS * LANE), 1) % LOW
    )

    def widen(value):
        return jnp.dot(value, spread, precision=HIGH, preferred_element_type=F32)

    ctf_wide = widen(ctf_ref[...])
    noise_wide = widen(jnp.broadcast_to(noise_ref[...], (8, CYCLES)))[:1]
    tau_wide = widen(jnp.broadcast_to(1.0 / tau_ref[...], (8, CYCLES)))[:1]
    prior = column_of(prior_ref[...].astype(F32), owned)

    def arrive(g):
        piece = part_of(g)
        for hop, copy in enumerate(direct[g]):
            copy.wait_recv()
            origin = lax.rem(row_id + n - 2 * (hop + 1), n)
            slot = every.at[origin, piece]
            relays[g][hop + 1] = send(
                slot, slot, {"img": partner}, relay_left.at[g, hop + 1], relay_sem.at[g, hop + 1]
            )

    def settle(g):
        for copy in relays[g]:
            copy.wait_recv()

    def setup():
        meta = every[:, 0].astype(F32).reshape(count, WIDE)
        group = iota((count, NDEF), 1).astype(F32)
        chosen = onehot(group == meta[:, :1])
        contrast = jnp.dot(chosen, ctf_wide, precision=HIGH, preferred_element_type=F32)
        square = contrast * contrast
        spot = iota((count, TABLE_ROWS), 1).astype(F32)
        lane = iota((count, LANE), 1)
        picks, terms = [], []
        for t in range(TRANS):
            dx = meta[:, 1 + t : 2 + t]
            dy = meta[:, 1 + TRANS + t : 2 + TRANS + t]
            index = (dx + REACH) * SIDE + (dy + REACH)
            picks.append(onehot((spot == index) | (spot == index + COMBOS)).astype(BF16))
            value = -(dx * dx + dy * dy) / (2.0 * offset_sigma * offset_sigma)
            terms.append(jnp.where(lane == 0, value, 0.0))
        coef = square / (2.0 * noise_wide)
        coef = jnp.concatenate([coef] * TRANS, axis=0)
        base = prior - lax.dot_general(power, coef, BY_LANE, precision=HIGH, preferred_element_type=F32)
        base = base + lax.dot_general(
            jnp.ones((owned, LANE), F32), jnp.concatenate(terms, axis=0), BY_LANE,
            precision=HIGH, preferred_element_type=F32,
        )
        return picks, contrast, square, contrast / noise_wide, base

    def build(g, picks, contrast, scaled, slot):
        bright = contrast[:, g * LANE : (g + 1) * LANE]
        scale = scaled[:, g * LANE : (g + 1) * LANE]
        for j in range(COLS):
            tile = g * COLS + j
            picture = every[:, 1 + tile].astype(F32).reshape(count, WIDE)
            real, imag = picture[:, :LANE], picture[:, LANE:]
            for t in range(TRANS):
                phase = jnp.dot(picks[t], table[tile], preferred_element_type=F32)
                cosine, sine = phase[:, :LANE], phase[:, LANE:]
                moved_real = real * cosine - imag * sine
                moved_imag = real * sine + imag * cosine
                span = slice(t * count, (t + 1) * count)
                inserted[tile, span, :LANE] = (moved_real * bright).astype(BF16)
                inserted[tile, span, LANE:] = (moved_imag * bright).astype(BF16)
                slot[span, j * WIDE : j * WIDE + LANE] = (moved_real * scale).astype(BF16)
                slot[span, j * WIDE + LANE : (j + 1) * WIDE] = (moved_imag * scale).astype(BF16)

    def score(g, slot):
        left = jnp.concatenate(
            [turned[g, (COLS - j) * step : (COLS - j) * step + height] for j in range(COLS)], axis=1
        )
        value = lax.dot_general(left, slot[...], BY_LANE, preferred_element_type=F32)
        if g == 0:
            acc[...] = value
        else:
            acc[...] += value

    loads[2].wait()
    keep.wait()
    arrive(0)
    settle(0)
    picks, contrast, square, scaled, base = setup()
    for g in range(GROUPS):
        if g + 1 < GROUPS:
            arrive(g + 1)
        if g:
            settle(g)
        build(g, picks, contrast, scaled, weighted[g % 2])
        if g:
            score(g - 1, weighted[(g - 1) % 2])
    score(GROUPS - 1, weighted[(GROUPS - 1) % 2])

    def over_shifts(value, combine):
        total = value
        for t in range(1, TRANS):
            total = combine(total, pltpu.roll(value, t * count, 1))
        return total

    peak = jnp.full((owned, rows), -jnp.inf, F32)
    for r in range(ROT):
        peak = jnp.maximum(peak, acc[r * owned : (r + 1) * owned])
    peak = jnp.max(peak + base, axis=0, keepdims=True)
    peak = over_shifts(jnp.broadcast_to(peak, (8, rows)), jnp.maximum)[:1]
    less = base - peak
    total = jnp.zeros((owned, rows), F32)
    for r in range(ROT):
        expo = jnp.exp(acc[r * owned : (r + 1) * owned] + less)
        acc[r * owned : (r + 1) * owned] = expo
        total = total + expo
    total = jnp.sum(total, axis=0, keepdims=True)
    total = over_shifts(jnp.broadcast_to(total, (8, rows)), jnp.add)[:1]
    stat[0:1] = peak[:, :width]
    stat[1:2] = total[:, :width]

    def send_all(src, dst, targets, left, landed):
        return [send(src, dst, peer, left.at[hop], landed.at[hop]) for hop, peer in enumerate(targets)]

    slot = stats.at[row_id, column_id]
    first = send_all(stat, slot, above, cls_left, cls_sem)
    keep = pltpu.make_async_copy(stat, slot, keep_sem.at[1])
    keep.start()
    keep.wait()
    for copy in first:
        copy.wait_recv()
    second = send_all(stats.at[row_id], stats.at[row_id], beside, img_left, img_sem)
    for copy in second:
        copy.wait_recv()

    entries = [stats[i, c] for i in range(n) for c in range(m)]
    top = entries[0]
    for entry in entries[1:]:
        top = jnp.maximum(top, entry)
    top = top[:1]
    whole = jnp.zeros((1, width), F32)
    for entry in entries:
        whole = whole + entry[1:2] * jnp.exp(entry[:1] - top)
    logs = jnp.broadcast_to(top + jnp.log(whole), (8, width))
    loglik_ref[...] = pltpu.roll(logs, width - row_id * local, 1)[:1, :local]
    factor = jnp.exp(stat[0:1] - top) / whole
    factor = jnp.concatenate([factor] * (rows // width), axis=1)

    summed = jnp.zeros((owned, rows), F32)
    for r in range(ROT):
        value = (acc[r * owned : (r + 1) * owned] * factor).astype(BF16)
        summed = summed + value.astype(F32)
        shift, q = r // MIX, r % MIX
        for spot in ((COLS - shift) % COLS, (COLS - shift) % COLS + COLS):
            post[spot * step + q * owned : spot * step + (q + 1) * owned] = value
    weight = jnp.sum(summed, axis=1, keepdims=True) * (1.0 / count)
    diagonal = iota((owned, owned), 0) == iota((owned, owned), 1)
    weight_ref[...] = jnp.sum(
        jnp.where(diagonal, jnp.broadcast_to(weight, (owned, owned)), 0.0), axis=0, keepdims=True
    )
    denom = jnp.dot(
        summed, jnp.concatenate([square] * TRANS, axis=0), precision=HIGH, preferred_element_type=F32
    )
    inverse = 1.0 / (denom + tau_wide)

    lane = iota((owned, LANE), 1)
    seg = iota((owned, LANE), 1) // SEG
    for g in range(GROUPS):
        left = jnp.concatenate(
            [post[(COLS - s) * step : (COLS - s) * step + height] for s in range(COLS)], axis=1
        )
        right = jnp.concatenate([inserted[g * COLS + s] for s in range(COLS)], axis=0)
        mixed[...] = jnp.dot(left, right, preferred_element_type=F32)
        scale = inverse[:, g * LANE : (g + 1) * LANE]
        spread_out = [[], []]
        for j in range(COLS):
            halves = []
            for p in range(2):
                half = slice(p * LANE, (p + 1) * LANE)
                value = mixed[j * step : j * step + owned, half]
                for q in range(1, MIX):
                    after = (j + 1) % COLS
                    here = pltpu.roll(mixed[j * step + q * owned : j * step + (q + 1) * owned, half], LANE - q * TURN, 1)
                    there = pltpu.roll(
                        mixed[after * step + q * owned : after * step + (q + 1) * owned, half], LANE - q * TURN, 1
                    )
                    value = value + jnp.where(lane < LANE - q * TURN, here, there)
                halves.append(value * scale)
            value = jnp.concatenate(halves, axis=0)
            high = value.astype(BF16)
            low = (value - high.astype(F32)).astype(BF16)
            value = jnp.dot(jnp.concatenate([high, low], axis=1), unblend[j % LOW], preferred_element_type=F32)
            for p in range(2):
                spread_out[p].append(value[p * owned : (p + 1) * owned])
        for p in range(2):
            for k in range(COLS):
                start = p * CYCLES * ANG + g * SPAN + k * LANE
                fresh_ref[:, start : start + LANE] = pick_segments(
                    [spread_out[p][(LOW * k + s) % COLS] for s in range(LOW)], seg
                )

    for copy in sum(direct, []) + sum(relays, []) + first + second:
        copy.wait_send()


def per_device(
    images, references, class_logprior, ctf_table, noise_power, tau_power, defocus, offsets
):
    n, m = lax.axis_size("img"), lax.axis_size("cls")
    local = images.shape[0]
    count = local * n
    rows = count * TRANS
    owned_true = references.shape[0]
    owned = -(-owned_true // 16) * 16
    spare = owned - owned_true
    width = max(count, LANE)
    height = ROT * owned
    vmem = pl.BlockSpec(memory_space=pltpu.VMEM)
    hbm = pl.BlockSpec(memory_space=pl.ANY)
    prior = class_logprior
    if spare:
        references = jnp.pad(references, ((0, spare), (0, 0)))
        prior = jnp.pad(class_logprior.astype(F32), (0, spare), constant_values=-1e30)

    dma = pltpu.SemaphoreType.DMA
    hops = n // 2 - 1
    fresh, weight, loglik = pl.pallas_call(
        lambda *refs: kernel(n, m, *refs),
        out_shape=(
            jax.ShapeDtypeStruct((owned, 2 * CYCLES * ANG), F32),
            jax.ShapeDtypeStruct((1, owned), F32),
            jax.ShapeDtypeStruct((1, local), F32),
        ),
        in_specs=[hbm, hbm] + [vmem] * 6 + [hbm],
        out_specs=(vmem,) * 3,
        scratch_shapes=[
            pltpu.VMEM((local, 2 * CYCLES * ANG), BF16),
            pltpu.VMEM((owned, 2 * CYCLES * ANG), BF16),
            pltpu.VMEM((TILES, TABLE_ROWS, WIDE), BF16),
            pltpu.VMEM((1 + TILES, local, WIDE), BF16),
            pltpu.VMEM((n, 1 + TILES, local, WIDE), BF16),
            pltpu.VMEM((COLS, 2 * GROUPS * owned, LANE), F32),
            pltpu.VMEM((LOW, LANE, LANE), BF16),
            pltpu.VMEM((LOW, WIDE, LANE), BF16),
            pltpu.VMEM((GROUPS, 2 * height, WIDE), BF16),
            pltpu.VMEM((rows, COLS * WIDE), BF16),
            pltpu.VMEM((rows, COLS * WIDE), BF16),
            pltpu.VMEM((TILES, rows, WIDE), BF16),
            pltpu.VMEM((height, rows), F32),
            pltpu.VMEM((2 * height, rows), BF16),
            pltpu.VMEM((height, WIDE), F32),
            pltpu.VMEM((2, width), F32),
            pltpu.VMEM((n, m, 2, width), F32),
            dma((3,)),
            dma((GROUPS, hops)),
            dma((GROUPS, hops)),
            dma((GROUPS, hops + 1)),
            dma((GROUPS, hops + 1)),
            dma((m - 1,)),
            dma((m - 1,)),
            dma((n - 1,)),
            dma((n - 1,)),
            dma((2,)),
        ],
        compiler_params=pltpu.CompilerParams(
            collective_id=0, has_side_effects=True, vmem_limit_bytes=60 * 1024 * 1024
        ),
        name="classify",
    )(
        images,
        references,
        prior[None],
        ctf_table,
        noise_power[None],
        tau_power[None],
        defocus[None],
        offsets.transpose(1, 2, 0),
        jnp.asarray(phase_rows()),
    )
    return fresh[:owned_true], weight[0, :owned_true], loglik[0]


def solution(mesh):
    return jax.shard_map(
        per_device,
        mesh=mesh,
        in_specs=(
            P("img", None),
            P(("img", "cls"), None),
            P(("img", "cls")),
            P(),
            P(),
            P(),
            P("img"),
            P("img", None, None),
        ),
        out_specs=(P(("img", "cls"), None), P(("img", "cls")), P("img")),
        check_vma=False,
    )
```

```python
import math

import jax
import jax.numpy as jnp
import numpy as np
from jax import lax
from jax.experimental import pallas as pl
from jax.experimental.pallas import tpu as pltpu
from jax.sharding import PartitionSpec as P

TRANS = 4
CYCLES = 32
ANG = 144
ROT = 36
NDEF = 16

STRIDE = ANG // ROT
REACH = 3
SIDE = 2 * REACH + 1
COMBOS = SIDE * SIDE
TABLE_ROWS = 112
HIGH = lax.Precision.HIGHEST
offset_sigma = 2.0

LANE = 128
LOW = 8
GROUPS = CYCLES // LOW
SPAN = LOW * ANG
COLS = SPAN // LANE
MIX = ROT // COLS
TURN = LANE // MIX
SEG = LANE // LOW
TILES = GROUPS * COLS
WIDE = 2 * LANE
BY_LANE = (((1,), (1,)), ((), ()))
F32 = jnp.float32
BF16 = jnp.bfloat16


def phase_rows():
    group = np.arange(GROUPS)[:, None, None]
    column = np.arange(COLS)[None, :, None]
    lane = np.arange(LANE)[None, None, :]
    radius = group * LOW + lane % LOW + 1.0
    theta = 2.0 * math.pi * (column * SEG + lane // LOW) / ANG
    freq_x = (radius * np.cos(theta)).reshape(TILES, 1, LANE)
    freq_y = (radius * np.sin(theta)).reshape(TILES, 1, LANE)
    combo = np.arange(COMBOS)[None, :, None]
    dx = combo // SIDE - REACH
    dy = combo % SIDE - REACH
    angle = -2.0 * math.pi * (dx * freq_x + dy * freq_y) / (2.0 * CYCLES)
    full = np.concatenate([np.cos(angle), np.sin(angle)], axis=2)
    high = full.astype(jnp.bfloat16)
    low = (full - high.astype(np.float64)).astype(jnp.bfloat16)
    table = np.zeros((TILES, TABLE_ROWS, WIDE), jnp.bfloat16)
    table[:, :COMBOS] = high
    table[:, COMBOS : 2 * COMBOS] = low
    return table


def iota(shape, dim):
    return lax.broadcasted_iota(jnp.int32, shape, dim)


def onehot(mask):
    return jnp.where(mask, 1.0, 0.0).astype(F32)


def column_of(row, size):
    square = jnp.broadcast_to(row, (size, size))
    return jnp.sum(
        jnp.where(iota((size, size), 0) == iota((size, size), 1), square, 0.0), axis=1, keepdims=True
    )


def pick_segments(sources, seg):
    value = sources[0]
    for s in range(1, LOW):
        value = jnp.where(seg == s, sources[s], value)
    return value


def natural_to_mixed(block, j, seg):
    sources = []
    for s in range(LOW):
        cycle = (s - j) % LOW
        n = (cycle * COLS + j - s) // LOW
        sources.append(block(n))
    return pick_segments(sources, seg)


def kernel(
    n, m,
    images_hbm, refs_hbm, prior_ref, ctf_ref, noise_ref, tau_ref, defocus_ref, offsets_ref, table_hbm,
    fresh_ref, weight_ref, loglik_ref,
    images_nat, refs_nat, table, own, every, spin, blend, unblend, turned, weighted_a, weighted_b, inserted,
    acc, post, mixed, scales, stat, stats,
    load_sem, left_sem, direct_sem, relay_left, relay_sem, stat_left, stat_sem, keep_sem, plane_sem,
):
    local = images_nat.shape[0]
    owned = refs_nat.shape[0]
    count = n * local
    rows = count * TRANS
    width = stat.shape[1]
    height = ROT * owned
    step = MIX * owned
    weighted = (weighted_a, weighted_b)

    row_id, column_id = lax.axis_index("img"), lax.axis_index("cls")
    partner = row_id + 1 - 2 * lax.rem(row_id, 2)
    peers = [lax.rem(row_id + 2 * hop, n) for hop in range(1, n // 2)]
    above = [{"cls": lax.rem(column_id + hop, m)} for hop in range(1, m)]
    beside = [{"img": lax.rem(row_id + hop, n)} for hop in range(1, n)]
    others = [
        {"img": lax.rem(row_id + i, n), "cls": lax.rem(column_id + c, m)}
        for i in range(n) for c in range(m) if i or c
    ]

    loads = [
        pltpu.make_async_copy(images_hbm, images_nat, load_sem.at[0]),
        pltpu.make_async_copy(refs_hbm, refs_nat, load_sem.at[1]),
        pltpu.make_async_copy(table_hbm, table, load_sem.at[2]),
    ]
    for copy in loads:
        copy.start()
    barrier = pltpu.get_barrier_semaphore()
    for peer in above + beside:
        pl.semaphore_signal(barrier, inc=1, device_id=peer, device_id_type=pl.DeviceIdType.MESH)

    def send(src, dst, peer, left, landed):
        copy = pltpu.make_async_remote_copy(
            src_ref=src, dst_ref=dst, send_sem=left, recv_sem=landed,
            device_id=peer, device_id_type=pl.DeviceIdType.MESH,
        )
        copy.start()
        return copy

    source = iota((LANE, LANE), 0)
    target = iota((LANE, LANE), 1)
    for j in range(LOW):
        place = (source % SEG) * LOW + (source // SEG + (LOW - j)) % LOW
        blend[j] = onehot(target == place).astype(BF16)
        place = (target % SEG) * LOW + (target // SEG + (LOW - j)) % LOW
        back = onehot(source == place).astype(BF16)
        unblend[j, :LANE] = back
        unblend[j, LANE:] = back

    meta = jnp.zeros((local, WIDE), F32)
    lane = iota((local, WIDE), 1)
    meta = jnp.where(lane == 0, column_of(defocus_ref[...].astype(F32), local), meta)
    for t in range(TRANS):
        for axis in range(2):
            value = column_of(offsets_ref[t, axis : axis + 1].astype(F32), local)
            meta = jnp.where(lane == 1 + t + axis * TRANS, value, meta)
    own[0] = meta.astype(BF16)

    def mix(nat, size, j):
        seg = iota((size, LANE), 1) // SEG
        parts = []
        for g in range(GROUPS):
            for p in range(2):
                start = p * CYCLES * ANG + g * SPAN

                def block(k, start=start):
                    return nat[:, start + k * LANE : start + (k + 1) * LANE].astype(F32)

                parts.append(natural_to_mixed(block, j, seg))
        stacked = jnp.concatenate(parts, axis=0).astype(BF16)
        return jnp.dot(stacked, blend[j % LOW], preferred_element_type=F32)

    loads[0].wait()
    for j in range(COLS):
        moved = mix(images_nat, local, j).astype(BF16)
        for g in range(GROUPS):
            for p in range(2):
                index = g * 2 + p
                own[1 + g * COLS + j, :, p * LANE : (p + 1) * LANE] = moved[
                    index * local : (index + 1) * local
                ]

    pl.semaphore_wait(barrier, n + m - 2)
    for peer in above:
        pl.semaphore_signal(plane_sem, inc=1, device_id=peer, device_id_type=pl.DeviceIdType.MESH)

    def part_of(g):
        return pl.ds(0, COLS + 1) if g == 0 else pl.ds(1 + g * COLS, COLS)

    direct = [[None] * len(peers) for _ in range(GROUPS)]
    relays = [[None] * (len(peers) + 1) for _ in range(GROUPS)]
    for g in range(GROUPS):
        piece = part_of(g)
        for hop, peer in enumerate(peers):
            direct[g][hop] = send(
                own.at[piece], every.at[row_id, piece], {"img": peer}, left_sem.at[g, hop], direct_sem.at[g, hop]
            )
        relays[g][0] = send(
            own.at[piece], every.at[row_id, piece], {"img": partner}, relay_left.at[g, 0], relay_sem.at[g, 0]
        )
    keep = pltpu.make_async_copy(own, every.at[row_id], keep_sem.at[0])
    keep.start()

    loads[1].wait()
    for j in range(COLS):
        spin[j] = mix(refs_nat, owned, j)
    lane = iota((2 * GROUPS * owned, LANE), 1)
    for q in range(MIX):
        before = pltpu.roll(spin[COLS - 1], q * TURN, 1) if q else None
        for j in range(COLS):
            if q:
                here = pltpu.roll(spin[j], q * TURN, 1)
                value = jnp.where(lane < q * TURN, before, here).astype(BF16)
                before = here
            else:
                value = spin[j].astype(BF16)
            for g in range(GROUPS):
                for p in range(2):
                    index = g * 2 + p
                    for spot in ((COLS - j) % COLS, (COLS - j) % COLS + COLS):
                        turned[
                            g, spot * step + q * owned : spot * step + (q + 1) * owned, p * LANE : (p + 1) * LANE
                        ] = value[index * owned : (index + 1) * owned]
    power = [jnp.zeros((owned, LANE), F32) for _ in range(GROUPS)]
    for j in range(COLS):
        for g in range(GROUPS):
            for p in range(2):
                index = g * 2 + p
                entry = spin[j, index * owned : (index + 1) * owned]
                power[g] = power[g] + entry * entry
    power = jnp.concatenate(power, axis=1)
    spread = onehot(
        iota((CYCLES, GROUPS * LANE), 0)
        == iota((CYCLES, GROUPS * LANE), 1) // LANE * LOW + iota((CYCLES, GROUPS * LANE), 1) % LOW
    )

    def widen(value):
        return jnp.dot(value, spread, precision=HIGH, preferred_element_type=F32)

    ctf_wide = widen(ctf_ref[...])
    noise_wide = widen(jnp.broadcast_to(noise_ref[...], (8, CYCLES)))[:1]
    tau_wide = widen(jnp.broadcast_to(1.0 / tau_ref[...], (8, CYCLES)))[:1]
    prior = column_of(prior_ref[...].astype(F32), owned)

    def arrive(g):
        piece = part_of(g)
        for hop, copy in enumerate(direct[g]):
            copy.wait_recv()
            origin = lax.rem(row_id + n - 2 * (hop + 1), n)
            slot = every.at[origin, piece]
            relays[g][hop + 1] = send(
                slot, slot, {"img": partner}, relay_left.at[g, hop + 1], relay_sem.at[g, hop + 1]
            )

    def settle(g):
        for copy in relays[g]:
            copy.wait_recv()

    def setup():
        meta = every[:, 0].astype(F32).reshape(count, WIDE)
        group = iota((count, NDEF), 1).astype(F32)
        chosen = onehot(group == meta[:, :1])
        contrast = jnp.dot(chosen, ctf_wide, precision=HIGH, preferred_element_type=F32)
        square = contrast * contrast
        spot = iota((count, TABLE_ROWS), 1).astype(F32)
        lane = iota((count, LANE), 1)
        picks, terms = [], []
        for t in range(TRANS):
            dx = meta[:, 1 + t : 2 + t]
            dy = meta[:, 1 + TRANS + t : 2 + TRANS + t]
            index = (dx + REACH) * SIDE + (dy + REACH)
            picks.append(onehot((spot == index) | (spot == index + COMBOS)).astype(BF16))
            value = -(dx * dx + dy * dy) / (2.0 * offset_sigma * offset_sigma)
            terms.append(jnp.where(lane == 0, value, 0.0))
        coef = square / (2.0 * noise_wide)
        coef = jnp.concatenate([coef] * TRANS, axis=0)
        base = prior - lax.dot_general(power, coef, BY_LANE, precision=HIGH, preferred_element_type=F32)
        base = base + lax.dot_general(
            jnp.ones((owned, LANE), F32), jnp.concatenate(terms, axis=0), BY_LANE,
            precision=HIGH, preferred_element_type=F32,
        )
        return picks, contrast, square, contrast / noise_wide, base

    def build(g, picks, contrast, scaled, slot):
        bright = contrast[:, g * LANE : (g + 1) * LANE]
        scale = scaled[:, g * LANE : (g + 1) * LANE]
        for j in range(COLS):
            tile = g * COLS + j
            picture = every[:, 1 + tile].astype(F32).reshape(count, WIDE)
            real, imag = picture[:, :LANE], picture[:, LANE:]
            for t in range(TRANS):
                phase = jnp.dot(picks[t], table[tile], preferred_element_type=F32)
                cosine, sine = phase[:, :LANE], phase[:, LANE:]
                moved_real = real * cosine - imag * sine
                moved_imag = real * sine + imag * cosine
                span = slice(t * count, (t + 1) * count)
                inserted[tile, span, :LANE] = (moved_real * bright).astype(BF16)
                inserted[tile, span, LANE:] = (moved_imag * bright).astype(BF16)
                slot[span, j * WIDE : j * WIDE + LANE] = (moved_real * scale).astype(BF16)
                slot[span, j * WIDE + LANE : (j + 1) * WIDE] = (moved_imag * scale).astype(BF16)

    def score(g, slot):
        left = jnp.concatenate(
            [turned[g, (COLS - j) * step : (COLS - j) * step + height] for j in range(COLS)], axis=1
        )
        value = lax.dot_general(left, slot[...], BY_LANE, preferred_element_type=F32)
        if g == 0:
            acc[...] = value
        else:
            acc[...] += value

    loads[2].wait()
    keep.wait()
    arrive(0)
    settle(0)
    picks, contrast, square, scaled, base = setup()
    for g in range(GROUPS):
        if g + 1 < GROUPS:
            arrive(g + 1)
        if g:
            settle(g)
        build(g, picks, contrast, scaled, weighted[g % 2])
        if g:
            score(g - 1, weighted[(g - 1) % 2])
    score(GROUPS - 1, weighted[(GROUPS - 1) % 2])

    def over_shifts(value, combine):
        total = value
        for t in range(1, TRANS):
            total = combine(total, pltpu.roll(value, t * count, 1))
        return total

    peak = jnp.full((owned, rows), -jnp.inf, F32)
    for r in range(ROT):
        peak = jnp.maximum(peak, acc[r * owned : (r + 1) * owned])
    peak = jnp.max(peak + base, axis=0, keepdims=True)
    peak = over_shifts(jnp.broadcast_to(peak, (8, rows)), jnp.maximum)[:1]
    less = base - peak
    total = jnp.zeros((owned, rows), F32)
    for r in range(ROT):
        expo = jnp.exp(acc[r * owned : (r + 1) * owned] + less)
        acc[r * owned : (r + 1) * owned] = expo
        total = total + expo
    total = jnp.sum(total, axis=0, keepdims=True)
    total = over_shifts(jnp.broadcast_to(total, (8, rows)), jnp.add)[:1]
    stat[0:1] = peak[:, :width]
    stat[1:2] = total[:, :width]

    stats[row_id, column_id] = stat[...]
    pl.semaphore_wait(plane_sem, m - 1)
    slot = stats.at[row_id, column_id]
    shared = [
        send(stat, slot, peer, stat_left.at[k], stat_sem.at[k]) for k, peer in enumerate(others)
    ]
    for copy in shared:
        copy.wait_recv()

    entries = [stats[i, c] for i in range(n) for c in range(m)]
    top = entries[0]
    for entry in entries[1:]:
        top = jnp.maximum(top, entry)
    top = top[:1]
    whole = jnp.zeros((1, width), F32)
    for entry in entries:
        whole = whole + entry[1:2] * jnp.exp(entry[:1] - top)
    logs = jnp.broadcast_to(top + jnp.log(whole), (8, width))
    loglik_ref[...] = pltpu.roll(logs, width - row_id * local, 1)[:1, :local]
    factor = jnp.exp(stat[0:1] - top) / whole
    factor = jnp.concatenate([factor] * (rows // width), axis=1)

    summed = jnp.zeros((owned, rows), F32)
    for r in range(ROT):
        value = (acc[r * owned : (r + 1) * owned] * factor).astype(BF16)
        summed = summed + value.astype(F32)
        shift, q = r // MIX, r % MIX
        for spot in ((COLS - shift) % COLS, (COLS - shift) % COLS + COLS):
            post[spot * step + q * owned : spot * step + (q + 1) * owned] = value
    weight = jnp.sum(summed, axis=1, keepdims=True) * (1.0 / count)
    diagonal = iota((owned, owned), 0) == iota((owned, owned), 1)
    weight_ref[...] = jnp.sum(
        jnp.where(diagonal, jnp.broadcast_to(weight, (owned, owned)), 0.0), axis=0, keepdims=True
    )
    denom = jnp.dot(
        summed, jnp.concatenate([square] * TRANS, axis=0), precision=HIGH, preferred_element_type=F32
    )
    inverse = 1.0 / (denom + tau_wide)

    lane = iota((owned, LANE), 1)
    seg = iota((owned, LANE), 1) // SEG
    for g in range(GROUPS):
        scales[g] = inverse[:, g * LANE : (g + 1) * LANE]

    @pl.loop(0, GROUPS)
    def _(g):
        left = jnp.concatenate(
            [post[(COLS - s) * step : (COLS - s) * step + height] for s in range(COLS)], axis=1
        )
        right = jnp.concatenate([inserted[g * COLS + s] for s in range(COLS)], axis=0)
        mixed[...] = jnp.dot(left, right, preferred_element_type=F32)
        scale = scales[g]
        spread_out = [[], []]
        for j in range(COLS):
            halves = []
            for p in range(2):
                half = slice(p * LANE, (p + 1) * LANE)
                value = mixed[j * step : j * step + owned, half]
                for q in range(1, MIX):
                    after = (j + 1) % COLS
                    here = pltpu.roll(mixed[j * step + q * owned : j * step + (q + 1) * owned, half], LANE - q * TURN, 1)
                    there = pltpu.roll(
                        mixed[after * step + q * owned : after * step + (q + 1) * owned, half], LANE - q * TURN, 1
                    )
                    value = value + jnp.where(lane < LANE - q * TURN, here, there)
                halves.append(value * scale)
            value = jnp.concatenate(halves, axis=0)
            high = value.astype(BF16)
            low = (value - high.astype(F32)).astype(BF16)
            value = jnp.dot(jnp.concatenate([high, low], axis=1), unblend[j % LOW], preferred_element_type=F32)
            for p in range(2):
                spread_out[p].append(value[p * owned : (p + 1) * owned])
        for p in range(2):
            for k in range(COLS):
                start = pl.multiple_of(g * SPAN + (p * CYCLES * ANG + k * LANE), LANE)
                fresh_ref[:, pl.ds(start, LANE)] = pick_segments(
                    [spread_out[p][(LOW * k + s) % COLS] for s in range(LOW)], seg
                )

    for copy in sum(direct, []) + sum(relays, []) + shared:
        copy.wait_send()


def publish(*refs):
    copies = [pltpu.make_async_copy(refs[k], refs[3 + k], refs[6].at[k]) for k in range(3)]
    for copy in copies:
        copy.start()
    for copy in copies:
        copy.wait()


def per_device(
    images, references, class_logprior, ctf_table, noise_power, tau_power, defocus, offsets
):
    n, m = lax.axis_size("img"), lax.axis_size("cls")
    local = images.shape[0]
    count = local * n
    rows = count * TRANS
    owned_true = references.shape[0]
    owned = -(-owned_true // 16) * 16
    spare = owned - owned_true
    width = max(count, LANE)
    height = ROT * owned
    vmem = pl.BlockSpec(memory_space=pltpu.VMEM)
    hbm = pl.BlockSpec(memory_space=pl.ANY)
    prior = class_logprior
    if spare:
        references = jnp.pad(references, ((0, spare), (0, 0)))
        prior = jnp.pad(class_logprior.astype(F32), (0, spare), constant_values=-1e30)

    dma = pltpu.SemaphoreType.DMA
    hops = n // 2 - 1
    fresh, weight, loglik = pl.pallas_call(
        lambda *refs: kernel(n, m, *refs),
        out_shape=(
            pltpu.VMEM((owned, 2 * CYCLES * ANG), F32),
            pltpu.VMEM((1, owned), F32),
            pltpu.VMEM((1, local), F32),
        ),
        in_specs=[hbm, hbm] + [vmem] * 6 + [hbm],
        out_specs=(vmem,) * 3,
        scratch_shapes=[
            pltpu.VMEM((local, 2 * CYCLES * ANG), BF16),
            pltpu.VMEM((owned, 2 * CYCLES * ANG), BF16),
            pltpu.VMEM((TILES, TABLE_ROWS, WIDE), BF16),
            pltpu.VMEM((1 + TILES, local, WIDE), BF16),
            pltpu.VMEM((n, 1 + TILES, local, WIDE), BF16),
            pltpu.VMEM((COLS, 2 * GROUPS * owned, LANE), F32),
            pltpu.VMEM((LOW, LANE, LANE), BF16),
            pltpu.VMEM((LOW, WIDE, LANE), BF16),
            pltpu.VMEM((GROUPS, 2 * height, WIDE), BF16),
            pltpu.VMEM((rows, COLS * WIDE), BF16),
            pltpu.VMEM((rows, COLS * WIDE), BF16),
            pltpu.VMEM((TILES, rows, WIDE), BF16),
            pltpu.VMEM((height, rows), F32),
            pltpu.VMEM((2 * height, rows), BF16),
            pltpu.VMEM((height, WIDE), F32),
            pltpu.VMEM((GROUPS, owned, LANE), F32),
            pltpu.VMEM((2, width), F32),
            pltpu.VMEM((n, m, 2, width), F32),
            dma((3,)),
            dma((GROUPS, hops)),
            dma((GROUPS, hops)),
            dma((GROUPS, hops + 1)),
            dma((GROUPS, hops + 1)),
            dma((n * m - 1,)),
            dma((n * m - 1,)),
            dma((1,)),
            pltpu.SemaphoreType.REGULAR,
        ],
        compiler_params=pltpu.CompilerParams(
            collective_id=0, has_side_effects=True, vmem_limit_bytes=60 * 1024 * 1024
        ),
        name="classify",
    )(
        images,
        references,
        prior[None],
        ctf_table,
        noise_power[None],
        tau_power[None],
        defocus[None],
        offsets.transpose(1, 2, 0),
        jnp.asarray(phase_rows()),
    )
    shapes = (fresh.shape, weight.shape, loglik.shape)
    fresh, weight, loglik = pl.pallas_call(
        publish,
        out_shape=tuple(jax.ShapeDtypeStruct(shape, F32) for shape in shapes),
        in_specs=[vmem] * 3,
        out_specs=(hbm,) * 3,
        scratch_shapes=[dma((3,))],
        compiler_params=pltpu.CompilerParams(vmem_limit_bytes=1024 * 1024),
        name="publish",
    )(fresh, weight, loglik)
    return fresh[:owned_true], weight[0, :owned_true], loglik[0]


def solution(mesh):
    return jax.shard_map(
        per_device,
        mesh=mesh,
        in_specs=(
            P("img", None),
            P(("img", "cls"), None),
            P(("img", "cls")),
            P(),
            P(),
            P(),
            P("img"),
            P("img", None, None),
        ),
        out_specs=(P(("img", "cls"), None), P(("img", "cls")), P("img")),
        check_vma=False,
    )
```

```python
import math

import jax
import jax.numpy as jnp
import numpy as np
from jax import lax
from jax.experimental import pallas as pl
from jax.experimental.pallas import tpu as pltpu
from jax.sharding import PartitionSpec as P

TRANS = 4
CYCLES = 32
ANG = 144
ROT = 36
NDEF = 16

STRIDE = ANG // ROT
REACH = 3
SIDE = 2 * REACH + 1
COMBOS = SIDE * SIDE
TABLE_ROWS = 112
HIGH = lax.Precision.HIGHEST
offset_sigma = 2.0

LANE = 128
LOW = 8
GROUPS = CYCLES // LOW
SPAN = LOW * ANG
COLS = SPAN // LANE
MIX = ROT // COLS
TURN = LANE // MIX
SEG = LANE // LOW
TILES = GROUPS * COLS
WIDE = 2 * LANE
CHUNK = 9
CHUNKS = TILES // CHUNK
BY_LANE = (((1,), (1,)), ((), ()))
F32 = jnp.float32
BF16 = jnp.bfloat16


def phase_rows():
    group = np.arange(GROUPS)[:, None, None]
    column = np.arange(COLS)[None, :, None]
    lane = np.arange(LANE)[None, None, :]
    radius = group * LOW + lane % LOW + 1.0
    theta = 2.0 * math.pi * (column * SEG + lane // LOW) / ANG
    freq_x = (radius * np.cos(theta)).reshape(TILES, 1, LANE)
    freq_y = (radius * np.sin(theta)).reshape(TILES, 1, LANE)
    combo = np.arange(COMBOS)[None, :, None]
    dx = combo // SIDE - REACH
    dy = combo % SIDE - REACH
    angle = -2.0 * math.pi * (dx * freq_x + dy * freq_y) / (2.0 * CYCLES)
    full = np.concatenate([np.cos(angle), np.sin(angle)], axis=2)
    high = full.astype(jnp.bfloat16)
    low = (full - high.astype(np.float64)).astype(jnp.bfloat16)
    table = np.zeros((TILES, TABLE_ROWS, WIDE), jnp.bfloat16)
    table[:, :COMBOS] = high
    table[:, COMBOS : 2 * COMBOS] = low
    return table


def iota(shape, dim):
    return lax.broadcasted_iota(jnp.int32, shape, dim)


def onehot(mask):
    return jnp.where(mask, 1.0, 0.0).astype(F32)


def column_of(row, size):
    square = jnp.broadcast_to(row, (size, size))
    return jnp.sum(
        jnp.where(iota((size, size), 0) == iota((size, size), 1), square, 0.0), axis=1, keepdims=True
    )


def pick_segments(sources, seg):
    value = sources[0]
    for s in range(1, LOW):
        value = jnp.where(seg == s, sources[s], value)
    return value


def natural_to_mixed(block, j, seg):
    sources = []
    for s in range(LOW):
        cycle = (s - j) % LOW
        n = (cycle * COLS + j - s) // LOW
        sources.append(block(n))
    return pick_segments(sources, seg)


def kernel(
    n, m,
    images_hbm, refs_hbm, prior_hbm, ctf_hbm, noise_hbm, tau_hbm, defocus_hbm, offsets_hbm, table_hbm,
    fresh_ref, weight_ref, loglik_ref,
    images_nat, refs_nat, prior_ref, ctf_ref, noise_ref, tau_ref, defocus_ref, offsets_ref, table, own, every, spin, blend, unblend, turned, weighted, inserted, own_meta, metas, picks, phases, bright, quiet,
    acc, post, mixed, inverses, stat, stats,
    load_sem, left_sem, direct_sem, relay_left, relay_sem, stat_left, stat_sem, meta_left, meta_sem, keep_sem, plane_sem,
):
    local = images_nat.shape[0]
    owned = refs_nat.shape[0]
    count = n * local
    rows = count * TRANS
    width = stat.shape[1]
    height = ROT * owned
    step = MIX * owned

    row_id, column_id = lax.axis_index("img"), lax.axis_index("cls")
    partner = row_id + 1 - 2 * lax.rem(row_id, 2)
    peers = [lax.rem(row_id + 2 * hop, n) for hop in range(1, n // 2)]
    above = [{"cls": lax.rem(column_id + hop, m)} for hop in range(1, m)]
    beside = [{"img": lax.rem(row_id + hop, n)} for hop in range(1, n)]
    others = [
        {"img": lax.rem(row_id + i, n), "cls": lax.rem(column_id + c, m)}
        for i in range(n) for c in range(m) if i or c
    ]

    barrier = pltpu.get_barrier_semaphore()
    for peer in above + beside:
        pl.semaphore_signal(barrier, inc=1, device_id=peer, device_id_type=pl.DeviceIdType.MESH)
    pairs = (
        (images_hbm, images_nat), (defocus_hbm, defocus_ref), (offsets_hbm, offsets_ref), (refs_hbm, refs_nat),
        (prior_hbm, prior_ref), (ctf_hbm, ctf_ref), (noise_hbm, noise_ref), (tau_hbm, tau_ref), (table_hbm, table),
    )
    loads = [pltpu.make_async_copy(src, dst, load_sem.at[k]) for k, (src, dst) in enumerate(pairs)]
    for copy in loads:
        copy.start()

    def send(src, dst, peer, left, landed):
        copy = pltpu.make_async_remote_copy(
            src_ref=src, dst_ref=dst, send_sem=left, recv_sem=landed,
            device_id=peer, device_id_type=pl.DeviceIdType.MESH,
        )
        copy.start()
        return copy

    source = iota((LANE, LANE), 0)
    target = iota((LANE, LANE), 1)
    for j in range(LOW):
        place = (source % SEG) * LOW + (source // SEG + (LOW - j)) % LOW
        blend[j] = onehot(target == place).astype(BF16)
        place = (target % SEG) * LOW + (target // SEG + (LOW - j)) % LOW
        back = onehot(source == place).astype(BF16)
        unblend[j, :LANE] = back
        unblend[j, LANE:] = back

    loads[1].wait()
    loads[2].wait()
    meta = jnp.zeros((local, LANE), F32)
    lane = iota((local, LANE), 1)
    meta = jnp.where(lane == 0, column_of(defocus_ref[...].astype(F32), local), meta)
    for t in range(TRANS):
        for axis in range(2):
            value = column_of(offsets_ref[t, axis : axis + 1].astype(F32), local)
            meta = jnp.where(lane == 1 + t + axis * TRANS, value, meta)
    own_meta[...] = meta.astype(BF16)

    def mix(nat, size, j):
        seg = iota((size, LANE), 1) // SEG
        parts = []
        for g in range(GROUPS):
            for p in range(2):
                start = p * CYCLES * ANG + g * SPAN

                def block(k, start=start):
                    return nat[:, start + k * LANE : start + (k + 1) * LANE].astype(F32)

                parts.append(natural_to_mixed(block, j, seg))
        stacked = jnp.concatenate(parts, axis=0).astype(BF16)
        return jnp.dot(stacked, blend[j % LOW], preferred_element_type=F32)

    loads[0].wait()
    for j in range(COLS):
        moved = mix(images_nat, local, j).astype(BF16)
        for g in range(GROUPS):
            for p in range(2):
                index = g * 2 + p
                own[g * COLS + j, :, p * LANE : (p + 1) * LANE] = moved[
                    index * local : (index + 1) * local
                ]

    pl.semaphore_wait(barrier, n + m - 2)
    for peer in above:
        pl.semaphore_signal(plane_sem, inc=1, device_id=peer, device_id_type=pl.DeviceIdType.MESH)

    def remote(src, dst, peer, left, landed):
        return pltpu.make_async_remote_copy(
            src_ref=src, dst_ref=dst, send_sem=left, recv_sem=landed,
            device_id=peer, device_id_type=pl.DeviceIdType.MESH,
        )

    def outward(c, hop):
        piece = pl.ds(c * CHUNK, CHUNK)
        return remote(
            own.at[piece], every.at[row_id, piece], {"img": peers[hop]}, left_sem.at[c, hop], direct_sem.at[c, hop]
        )

    def relay(c, hop):
        piece = pl.ds(c * CHUNK, CHUNK)
        if hop == 0:
            src, dst = own.at[piece], every.at[row_id, piece]
        else:
            src = dst = every.at[lax.rem(row_id + n - 2 * hop, n), piece]
        return remote(src, dst, {"img": partner}, relay_left.at[c, hop], relay_sem.at[c, hop])

    def titles(hop):
        return remote(own_meta, metas.at[row_id], beside[hop], meta_left.at[hop], meta_sem.at[hop])

    hops = len(peers)
    for hop in range(n - 1):
        titles(hop).start()
    for c in range(CHUNKS):
        for hop in range(hops):
            outward(c, hop).start()
        relay(c, 0).start()
    keeps = [
        pltpu.make_async_copy(own, every.at[row_id], keep_sem.at[0]),
        pltpu.make_async_copy(own_meta, metas.at[row_id], keep_sem.at[1]),
    ]
    for copy in keeps:
        copy.start()
    acc[...] = jnp.zeros(acc.shape, F32)
    loads[3].wait()
    for j in range(COLS):
        spin[j] = mix(refs_nat, owned, j)
    lane = iota((2 * GROUPS * owned, LANE), 1)
    for q in range(MIX):
        before = pltpu.roll(spin[COLS - 1], q * TURN, 1) if q else None
        for j in range(COLS):
            if q:
                here = pltpu.roll(spin[j], q * TURN, 1)
                value = jnp.where(lane < q * TURN, before, here).astype(BF16)
                before = here
            else:
                value = spin[j].astype(BF16)
            for g in range(GROUPS):
                for p in range(2):
                    index = g * 2 + p
                    for spot in ((COLS - j) % COLS, (COLS - j) % COLS + COLS):
                        turned[
                            g, spot * step + q * owned : spot * step + (q + 1) * owned, p * LANE : (p + 1) * LANE
                        ] = value[index * owned : (index + 1) * owned]
    power = [jnp.zeros((owned, LANE), F32) for _ in range(GROUPS)]
    for j in range(COLS):
        for g in range(GROUPS):
            for p in range(2):
                index = g * 2 + p
                entry = spin[j, index * owned : (index + 1) * owned]
                power[g] = power[g] + entry * entry
    power = jnp.concatenate(power, axis=1)
    spread = onehot(
        iota((CYCLES, GROUPS * LANE), 0)
        == iota((CYCLES, GROUPS * LANE), 1) // LANE * LOW + iota((CYCLES, GROUPS * LANE), 1) % LOW
    )

    def widen(value):
        return jnp.dot(value, spread, precision=HIGH, preferred_element_type=F32)

    for copy in loads[4:8]:
        copy.wait()
    ctf_wide = widen(ctf_ref[...])
    noise_wide = widen(jnp.broadcast_to(noise_ref[...], (8, CYCLES)))[:1]
    tau_wide = widen(jnp.broadcast_to(1.0 / tau_ref[...], (8, CYCLES)))[:1]
    prior = column_of(prior_ref[...].astype(F32), owned)

    def arrive(c):
        for hop in range(hops):
            outward(c, hop).wait_recv()
            relay(c, hop + 1).start()

    def settle(c):
        for hop in range(hops + 1):
            relay(c, hop).wait_recv()

    def setup():
        meta = metas[...].astype(F32).reshape(count, LANE)
        group = iota((count, NDEF), 1).astype(F32)
        chosen = onehot(group == meta[:, :1])
        contrast = jnp.dot(chosen, ctf_wide, precision=HIGH, preferred_element_type=F32)
        square = contrast * contrast
        spot = iota((count, TABLE_ROWS), 1).astype(F32)
        lane = iota((count, LANE), 1)
        terms = []
        for t in range(TRANS):
            dx = meta[:, 1 + t : 2 + t]
            dy = meta[:, 1 + TRANS + t : 2 + TRANS + t]
            index = (dx + REACH) * SIDE + (dy + REACH)
            picks[t * count : (t + 1) * count] = onehot((spot == index) | (spot == index + COMBOS)).astype(BF16)
            value = -(dx * dx + dy * dy) / (2.0 * offset_sigma * offset_sigma)
            terms.append(jnp.where(lane == 0, value, 0.0))
        coef = square / (2.0 * noise_wide)
        coef = jnp.concatenate([coef] * TRANS, axis=0)
        base = prior - lax.dot_general(power, coef, BY_LANE, precision=HIGH, preferred_element_type=F32)
        base = base + lax.dot_general(
            jnp.ones((owned, LANE), F32), jnp.concatenate(terms, axis=0), BY_LANE,
            precision=HIGH, preferred_element_type=F32,
        )
        calm = 1.0 / noise_wide
        for g in range(GROUPS):
            bright[g] = contrast[:, g * LANE : (g + 1) * LANE]
            quiet[g : g + 1] = calm[:, g * LANE : (g + 1) * LANE]
        return square, base

    def prepare(begin, end):
        @pl.loop(begin // 6, end // 6)
        def _(block):
            for place in range(6):
                tile = block * 6 + place
                phases[tile] = jnp.dot(picks[...], table[tile], preferred_element_type=F32)

    def shifted(tile):
        light = bright[lax.div(tile, COLS)]
        picture = every[:, tile].astype(F32).reshape(count, WIDE)
        real, imag = picture[:, :LANE] * light, picture[:, LANE:] * light
        for t in range(TRANS):
            span = slice(t * count, (t + 1) * count)
            cosine, sine = phases[tile, span, :LANE], phases[tile, span, LANE:]
            yield span, real * cosine - imag * sine, real * sine + imag * cosine

    def build(tile, place, slot):
        calm = quiet[pl.ds(lax.div(tile, COLS), 1)]
        for span, real, imag in shifted(tile):
            inserted[tile, span, :LANE] = real.astype(BF16)
            inserted[tile, span, LANE:] = imag.astype(BF16)
            slot[span, place * WIDE : place * WIDE + LANE] = (real * calm).astype(BF16)
            slot[span, place * WIDE + LANE : (place + 1) * WIDE] = (imag * calm).astype(BF16)

    loads[8].wait()
    for copy in keeps:
        copy.wait()
    for hop in range(n - 1):
        titles(hop).wait_recv()
    square, base = setup()
    prepare(0, TILES // 2)
    arrive(0)
    prepare(TILES // 2, TILES)

    @pl.loop(0, CHUNKS)
    def _(c):
        @pl.when(c + 1 < CHUNKS)
        def _():
            arrive(c + 1)

        settle(c)
        lefts = []
        for place in range(CHUNK):
            tile = c * CHUNK + place
            build(tile, place, weighted)
            g, j = lax.div(tile, COLS), lax.rem(tile, COLS)
            lefts.append(turned[g, pl.ds(pl.multiple_of((COLS - j) * step, step), height)])
        acc[...] += lax.dot_general(
            jnp.concatenate(lefts, axis=1), weighted[...], BY_LANE, preferred_element_type=F32
        )

    def over_shifts(value, combine):
        total = value
        for t in range(1, TRANS):
            total = combine(total, pltpu.roll(value, t * count, 1))
        return total

    peak = jnp.full((owned, rows), -jnp.inf, F32)
    for r in range(ROT):
        peak = jnp.maximum(peak, acc[r * owned : (r + 1) * owned])
    peak = jnp.max(peak + base, axis=0, keepdims=True)
    peak = over_shifts(jnp.broadcast_to(peak, (8, rows)), jnp.maximum)[:1]
    less = base - peak
    total = jnp.zeros((owned, rows), F32)
    for r in range(ROT):
        expo = jnp.exp(acc[r * owned : (r + 1) * owned] + less)
        acc[r * owned : (r + 1) * owned] = expo
        total = total + expo
    total = jnp.sum(total, axis=0, keepdims=True)
    total = over_shifts(jnp.broadcast_to(total, (8, rows)), jnp.add)[:1]
    stat[0:1] = peak[:, :width]
    stat[1:2] = total[:, :width]

    stats[row_id, column_id] = stat[...]
    pl.semaphore_wait(plane_sem, m - 1)
    slot = stats.at[row_id, column_id]
    shared = [
        send(stat, slot, peer, stat_left.at[k], stat_sem.at[k]) for k, peer in enumerate(others)
    ]
    for copy in shared:
        copy.wait_recv()

    entries = [stats[i, c] for i in range(n) for c in range(m)]
    top = entries[0]
    for entry in entries[1:]:
        top = jnp.maximum(top, entry)
    top = top[:1]
    whole = jnp.zeros((1, width), F32)
    for entry in entries:
        whole = whole + entry[1:2] * jnp.exp(entry[:1] - top)
    logs = jnp.broadcast_to(top + jnp.log(whole), (8, width))
    loglik_ref[...] = pltpu.roll(logs, width - row_id * local, 1)[:1, :local]
    factor = jnp.exp(stat[0:1] - top) / whole
    factor = jnp.concatenate([factor] * (rows // width), axis=1)

    summed = jnp.zeros((owned, rows), F32)
    for r in range(ROT):
        value = (acc[r * owned : (r + 1) * owned] * factor).astype(BF16)
        summed = summed + value.astype(F32)
        shift, q = r // MIX, r % MIX
        for spot in ((COLS - shift) % COLS, (COLS - shift) % COLS + COLS):
            post[spot * step + q * owned : spot * step + (q + 1) * owned] = value
    weight = jnp.sum(summed, axis=1, keepdims=True) * (1.0 / count)
    diagonal = iota((owned, owned), 0) == iota((owned, owned), 1)
    weight_ref[...] = jnp.sum(
        jnp.where(diagonal, jnp.broadcast_to(weight, (owned, owned)), 0.0), axis=0, keepdims=True
    )
    denom = jnp.dot(
        summed, jnp.concatenate([square] * TRANS, axis=0), precision=HIGH, preferred_element_type=F32
    )
    inverse = 1.0 / (denom + tau_wide)

    lane = iota((owned, LANE), 1)
    seg = iota((owned, LANE), 1) // SEG
    for g in range(GROUPS):
        inverses[g] = inverse[:, g * LANE : (g + 1) * LANE]

    def insert(g):
        left = jnp.concatenate(
            [post[(COLS - s) * step : (COLS - s) * step + height] for s in range(COLS)], axis=1
        )
        right = jnp.concatenate([inserted[g * COLS + s] for s in range(COLS)], axis=0)
        return jnp.dot(left, right, preferred_element_type=F32)

    def finish(g):
        scale = inverses[g]
        spread_out = [[], []]
        for j in range(COLS):
            halves = []
            for p in range(2):
                half = slice(p * LANE, (p + 1) * LANE)
                value = mixed[j * step : j * step + owned, half]
                for q in range(1, MIX):
                    after = (j + 1) % COLS
                    here = pltpu.roll(mixed[j * step + q * owned : j * step + (q + 1) * owned, half], LANE - q * TURN, 1)
                    there = pltpu.roll(
                        mixed[after * step + q * owned : after * step + (q + 1) * owned, half], LANE - q * TURN, 1
                    )
                    value = value + jnp.where(lane < LANE - q * TURN, here, there)
                halves.append(value * scale)
            value = jnp.concatenate(halves, axis=0)
            high = value.astype(BF16)
            low = (value - high.astype(F32)).astype(BF16)
            value = jnp.dot(jnp.concatenate([high, low], axis=1), unblend[j % LOW], preferred_element_type=F32)
            for p in range(2):
                spread_out[p].append(value[p * owned : (p + 1) * owned])
        for p in range(2):
            for k in range(COLS):
                start = g * SPAN + (p * CYCLES * ANG + k * LANE)
                if not isinstance(g, int):
                    start = pl.multiple_of(start, LANE)
                fresh_ref[:, pl.ds(start, LANE)] = pick_segments(
                    [spread_out[p][(LOW * k + s) % COLS] for s in range(LOW)], seg
                )

    mixed[...] = insert(0)

    @pl.loop(1, GROUPS)
    def _(g):
        value = insert(g)
        finish(g - 1)
        mixed[...] = value

    finish(GROUPS - 1)

    for copy in shared + [titles(hop) for hop in range(n - 1)]:
        copy.wait_send()

    @pl.loop(0, CHUNKS)
    def _(c):
        for hop in range(hops):
            outward(c, hop).wait_send()
        for hop in range(hops + 1):
            relay(c, hop).wait_send()


def publish(*refs):
    copies = [pltpu.make_async_copy(refs[k], refs[3 + k], refs[6].at[k]) for k in range(3)]
    for copy in copies:
        copy.start()
    for copy in copies:
        copy.wait()


def per_device(
    images, references, class_logprior, ctf_table, noise_power, tau_power, defocus, offsets
):
    n, m = lax.axis_size("img"), lax.axis_size("cls")
    local = images.shape[0]
    count = local * n
    rows = count * TRANS
    owned_true = references.shape[0]
    owned = -(-owned_true // 16) * 16
    spare = owned - owned_true
    width = max(count, LANE)
    height = ROT * owned
    vmem = pl.BlockSpec(memory_space=pltpu.VMEM)
    hbm = pl.BlockSpec(memory_space=pl.ANY)
    prior = class_logprior
    if spare:
        references = jnp.pad(references, ((0, spare), (0, 0)))
        prior = jnp.pad(class_logprior.astype(F32), (0, spare), constant_values=-1e30)

    dma = pltpu.SemaphoreType.DMA
    hops = n // 2 - 1
    fresh, weight, loglik = pl.pallas_call(
        lambda *refs: kernel(n, m, *refs),
        out_shape=(
            pltpu.VMEM((owned, 2 * CYCLES * ANG), F32),
            pltpu.VMEM((1, owned), F32),
            pltpu.VMEM((1, local), F32),
        ),
        in_specs=[hbm] * 9,
        out_specs=(vmem,) * 3,
        scratch_shapes=[
            pltpu.VMEM((local, 2 * CYCLES * ANG), BF16),
            pltpu.VMEM((owned, 2 * CYCLES * ANG), BF16),
            pltpu.VMEM((1, owned), prior.dtype),
            pltpu.VMEM(ctf_table.shape, F32),
            pltpu.VMEM((1, CYCLES), F32),
            pltpu.VMEM((1, CYCLES), F32),
            pltpu.VMEM((1, local), jnp.int32),
            pltpu.VMEM((TRANS, 2, local), jnp.int32),
            pltpu.VMEM((TILES, TABLE_ROWS, WIDE), BF16),
            pltpu.VMEM((TILES, local, WIDE), BF16),
            pltpu.VMEM((n, TILES, local, WIDE), BF16),
            pltpu.VMEM((COLS, 2 * GROUPS * owned, LANE), F32),
            pltpu.VMEM((LOW, LANE, LANE), BF16),
            pltpu.VMEM((LOW, WIDE, LANE), BF16),
            pltpu.VMEM((GROUPS, 2 * height, WIDE), BF16),
            pltpu.VMEM((rows, CHUNK * WIDE), BF16),
            pltpu.VMEM((TILES, rows, WIDE), BF16),
            pltpu.VMEM((local, LANE), BF16),
            pltpu.VMEM((n, local, LANE), BF16),
            pltpu.VMEM((rows, TABLE_ROWS), BF16),
            pltpu.VMEM((TILES, rows, WIDE), F32),
            pltpu.VMEM((GROUPS, count, LANE), F32),
            pltpu.VMEM((GROUPS, LANE), F32),
            pltpu.VMEM((height, rows), F32),
            pltpu.VMEM((2 * height, rows), BF16),
            pltpu.VMEM((height, WIDE), F32),
            pltpu.VMEM((GROUPS, owned, LANE), F32),
            pltpu.VMEM((2, width), F32),
            pltpu.VMEM((n, m, 2, width), F32),
            dma((9,)),
            dma((CHUNKS, hops)),
            dma((CHUNKS, hops)),
            dma((CHUNKS, hops + 1)),
            dma((CHUNKS, hops + 1)),
            dma((n * m - 1,)),
            dma((n * m - 1,)),
            dma((n - 1,)),
            dma((n - 1,)),
            dma((2,)),
            pltpu.SemaphoreType.REGULAR,
        ],
        compiler_params=pltpu.CompilerParams(
            collective_id=0, has_side_effects=True, vmem_limit_bytes=60 * 1024 * 1024
        ),
        name="classify",
    )(
        images,
        references,
        prior[None],
        ctf_table,
        noise_power[None],
        tau_power[None],
        defocus[None],
        offsets.transpose(1, 2, 0),
        jnp.asarray(phase_rows()),
    )
    shapes = (fresh.shape, weight.shape, loglik.shape)
    fresh, weight, loglik = pl.pallas_call(
        publish,
        out_shape=tuple(jax.ShapeDtypeStruct(shape, F32) for shape in shapes),
        in_specs=[vmem] * 3,
        out_specs=(hbm,) * 3,
        scratch_shapes=[dma((3,))],
        compiler_params=pltpu.CompilerParams(vmem_limit_bytes=1024 * 1024),
        name="publish",
    )(fresh, weight, loglik)
    return fresh[:owned_true], weight[0, :owned_true], loglik[0]


def solution(mesh):
    return jax.shard_map(
        per_device,
        mesh=mesh,
        in_specs=(
            P("img", None),
            P(("img", "cls"), None),
            P(("img", "cls")),
            P(),
            P(),
            P(),
            P("img"),
            P("img", None, None),
        ),
        out_specs=(P(("img", "cls"), None), P(("img", "cls")), P("img")),
        check_vma=False,
    )
```

```python
import math

import jax
import jax.numpy as jnp
import numpy as np
from jax import lax
from jax.experimental import pallas as pl
from jax.experimental.pallas import tpu as pltpu
from jax.sharding import PartitionSpec as P

TRANS = 4
CYCLES = 32
ANG = 144
ROT = 36
NDEF = 16

STRIDE = ANG // ROT
REACH = 3
SIDE = 2 * REACH + 1
COMBOS = SIDE * SIDE
TABLE_ROWS = 112
HIGH = lax.Precision.HIGHEST
offset_sigma = 2.0

LANE = 128
LOW = 8
GROUPS = CYCLES // LOW
SPAN = LOW * ANG
COLS = SPAN // LANE
MIX = ROT // COLS
TURN = LANE // MIX
SEG = LANE // LOW
TILES = GROUPS * COLS
WIDE = 2 * LANE
CHUNK = 9
CHUNKS = TILES // CHUNK
BY_LANE = (((1,), (1,)), ((), ()))
F32 = jnp.float32
BF16 = jnp.bfloat16


def phase_rows():
    group = np.arange(GROUPS)[:, None, None]
    column = np.arange(COLS)[None, :, None]
    lane = np.arange(LANE)[None, None, :]
    radius = group * LOW + lane % LOW + 1.0
    theta = 2.0 * math.pi * (column * SEG + lane // LOW) / ANG
    freq_x = (radius * np.cos(theta)).reshape(TILES, 1, LANE)
    freq_y = (radius * np.sin(theta)).reshape(TILES, 1, LANE)
    combo = np.arange(COMBOS)[None, :, None]
    dx = combo // SIDE - REACH
    dy = combo % SIDE - REACH
    angle = -2.0 * math.pi * (dx * freq_x + dy * freq_y) / (2.0 * CYCLES)
    full = np.concatenate([np.cos(angle), np.sin(angle)], axis=2)
    high = full.astype(jnp.bfloat16)
    low = (full - high.astype(np.float64)).astype(jnp.bfloat16)
    table = np.zeros((TILES, TABLE_ROWS, WIDE), jnp.bfloat16)
    table[:, :COMBOS] = high
    table[:, COMBOS : 2 * COMBOS] = low
    return table


def iota(shape, dim):
    return lax.broadcasted_iota(jnp.int32, shape, dim)


def onehot(mask):
    return jnp.where(mask, 1.0, 0.0).astype(F32)


def column_of(row, size):
    square = jnp.broadcast_to(row, (size, size))
    return jnp.sum(
        jnp.where(iota((size, size), 0) == iota((size, size), 1), square, 0.0), axis=1, keepdims=True
    )


def pick_segments(sources, seg):
    value = sources[0]
    for s in range(1, LOW):
        value = jnp.where(seg == s, sources[s], value)
    return value


def natural_to_mixed(block, j, seg):
    sources = []
    for s in range(LOW):
        cycle = (s - j) % LOW
        n = (cycle * COLS + j - s) // LOW
        sources.append(block(n))
    return pick_segments(sources, seg)


def kernel(
    n, m,
    images_hbm, refs_hbm, prior_hbm, ctf_hbm, noise_hbm, tau_hbm, defocus_hbm, offsets_hbm, table_hbm,
    fresh_ref, weight_ref, loglik_ref,
    images_nat, refs_nat, prior_ref, ctf_ref, noise_ref, tau_ref, defocus_ref, offsets_ref, table, own, every, spin, blend, unblend, turned, weighted, inserted, own_meta, metas, picks, phases, bright, quiet,
    acc, post, mixed, inverses, stat, stats,
    load_sem, left_sem, direct_sem, relay_left, relay_sem, stat_left, stat_sem, meta_left, meta_sem, keep_sem, plane_sem,
):
    local = images_nat.shape[0]
    owned = refs_nat.shape[0]
    count = n * local
    rows = count * TRANS
    width = stat.shape[1]
    height = ROT * owned
    step = MIX * owned

    row_id, column_id = lax.axis_index("img"), lax.axis_index("cls")
    partner = row_id + 1 - 2 * lax.rem(row_id, 2)
    peers = [lax.rem(row_id + 2 * hop, n) for hop in range(1, n // 2)]
    above = [{"cls": lax.rem(column_id + hop, m)} for hop in range(1, m)]
    beside = [{"img": lax.rem(row_id + hop, n)} for hop in range(1, n)]
    others = [
        {"img": lax.rem(row_id + i, n), "cls": lax.rem(column_id + c, m)}
        for i in range(n) for c in range(m) if i or c
    ]

    barrier = pltpu.get_barrier_semaphore()
    for peer in above + beside:
        pl.semaphore_signal(barrier, inc=1, device_id=peer, device_id_type=pl.DeviceIdType.MESH)
    pairs = (
        (images_hbm, images_nat), (defocus_hbm, defocus_ref), (offsets_hbm, offsets_ref), (refs_hbm, refs_nat),
        (prior_hbm, prior_ref), (ctf_hbm, ctf_ref), (noise_hbm, noise_ref), (tau_hbm, tau_ref), (table_hbm, table),
    )
    loads = [pltpu.make_async_copy(src, dst, load_sem.at[k]) for k, (src, dst) in enumerate(pairs)]
    for copy in loads:
        copy.start()

    def send(src, dst, peer, left, landed):
        copy = pltpu.make_async_remote_copy(
            src_ref=src, dst_ref=dst, send_sem=left, recv_sem=landed,
            device_id=peer, device_id_type=pl.DeviceIdType.MESH,
        )
        copy.start()
        return copy

    source = iota((LANE, LANE), 0)
    target = iota((LANE, LANE), 1)
    for j in range(LOW):
        place = (source % SEG) * LOW + (source // SEG + (LOW - j)) % LOW
        blend[j] = onehot(target == place).astype(BF16)
        place = (target % SEG) * LOW + (target // SEG + (LOW - j)) % LOW
        back = onehot(source == place).astype(BF16)
        unblend[j, :LANE] = back
        unblend[j, LANE:] = back

    loads[1].wait()
    loads[2].wait()
    meta = jnp.zeros((local, LANE), F32)
    lane = iota((local, LANE), 1)
    meta = jnp.where(lane == 0, column_of(defocus_ref[...].astype(F32), local), meta)
    for t in range(TRANS):
        for axis in range(2):
            value = column_of(offsets_ref[t, axis : axis + 1].astype(F32), local)
            meta = jnp.where(lane == 1 + t + axis * TRANS, value, meta)
    own_meta[...] = meta.astype(BF16)

    def mix(nat, size, j):
        seg = iota((size, LANE), 1) // SEG
        parts = []
        for g in range(GROUPS):
            for p in range(2):
                start = p * CYCLES * ANG + g * SPAN

                def block(k, start=start):
                    return nat[:, start + k * LANE : start + (k + 1) * LANE].astype(F32)

                parts.append(natural_to_mixed(block, j, seg))
        stacked = jnp.concatenate(parts, axis=0).astype(BF16)
        return jnp.dot(stacked, blend[j % LOW], preferred_element_type=F32)

    loads[0].wait()
    for j in range(COLS):
        moved = mix(images_nat, local, j).astype(BF16)
        for g in range(GROUPS):
            for p in range(2):
                index = g * 2 + p
                own[g * COLS + j, :, p * LANE : (p + 1) * LANE] = moved[
                    index * local : (index + 1) * local
                ]

    pl.semaphore_wait(barrier, n + m - 2)
    for peer in above:
        pl.semaphore_signal(plane_sem, inc=1, device_id=peer, device_id_type=pl.DeviceIdType.MESH)

    def remote(src, dst, peer, left, landed):
        return pltpu.make_async_remote_copy(
            src_ref=src, dst_ref=dst, send_sem=left, recv_sem=landed,
            device_id=peer, device_id_type=pl.DeviceIdType.MESH,
        )

    def outward(c, hop):
        piece = pl.ds(c * CHUNK, CHUNK)
        return remote(
            own.at[piece], every.at[row_id, piece], {"img": peers[hop]}, left_sem.at[c, hop], direct_sem.at[c, hop]
        )

    def relay(c, hop):
        piece = pl.ds(c * CHUNK, CHUNK)
        if hop == 0:
            src, dst = own.at[piece], every.at[row_id, piece]
        else:
            src = dst = every.at[lax.rem(row_id + n - 2 * hop, n), piece]
        return remote(src, dst, {"img": partner}, relay_left.at[c, hop], relay_sem.at[c, hop])

    def titles(hop):
        return remote(own_meta, metas.at[row_id], beside[hop], meta_left.at[hop], meta_sem.at[hop])

    hops = len(peers)
    for hop in range(n - 1):
        titles(hop).start()
    for c in range(CHUNKS):
        for hop in range(hops):
            outward(c, hop).start()
        relay(c, 0).start()
    keeps = [
        pltpu.make_async_copy(own, every.at[row_id], keep_sem.at[0]),
        pltpu.make_async_copy(own_meta, metas.at[row_id], keep_sem.at[1]),
    ]
    for copy in keeps:
        copy.start()
    acc[...] = jnp.zeros(acc.shape, F32)
    loads[3].wait()
    for j in range(COLS):
        spin[j] = mix(refs_nat, owned, j)
    lane = iota((2 * GROUPS * owned, LANE), 1)
    for q in range(MIX):
        before = pltpu.roll(spin[COLS - 1], q * TURN, 1) if q else None
        for j in range(COLS):
            if q:
                here = pltpu.roll(spin[j], q * TURN, 1)
                value = jnp.where(lane < q * TURN, before, here).astype(BF16)
                before = here
            else:
                value = spin[j].astype(BF16)
            for g in range(GROUPS):
                for p in range(2):
                    index = g * 2 + p
                    for spot in ((COLS - j) % COLS, (COLS - j) % COLS + COLS):
                        turned[
                            g, spot * step + q * owned : spot * step + (q + 1) * owned, p * LANE : (p + 1) * LANE
                        ] = value[index * owned : (index + 1) * owned]
    power = [jnp.zeros((owned, LANE), F32) for _ in range(GROUPS)]
    for j in range(COLS):
        for g in range(GROUPS):
            for p in range(2):
                index = g * 2 + p
                entry = spin[j, index * owned : (index + 1) * owned]
                power[g] = power[g] + entry * entry
    power = jnp.concatenate(power, axis=1)
    spread = onehot(
        iota((CYCLES, GROUPS * LANE), 0)
        == iota((CYCLES, GROUPS * LANE), 1) // LANE * LOW + iota((CYCLES, GROUPS * LANE), 1) % LOW
    )

    def widen(value):
        return jnp.dot(value, spread, precision=HIGH, preferred_element_type=F32)

    for copy in loads[4:8]:
        copy.wait()
    ctf_wide = widen(ctf_ref[...])
    noise_wide = widen(jnp.broadcast_to(noise_ref[...], (8, CYCLES)))[:1]
    tau_wide = widen(jnp.broadcast_to(1.0 / tau_ref[...], (8, CYCLES)))[:1]
    prior = column_of(prior_ref[...].astype(F32), owned)

    def arrive(c):
        for hop in range(hops):
            outward(c, hop).wait_recv()
            relay(c, hop + 1).start()

    def settle(c):
        for hop in range(hops + 1):
            relay(c, hop).wait_recv()

    def setup():
        meta = metas[...].astype(F32).reshape(count, LANE)
        group = iota((count, NDEF), 1).astype(F32)
        chosen = onehot(group == meta[:, :1])
        contrast = jnp.dot(chosen, ctf_wide, precision=HIGH, preferred_element_type=F32)
        square = contrast * contrast
        spot = iota((count, TABLE_ROWS), 1).astype(F32)
        lane = iota((count, LANE), 1)
        terms = []
        for t in range(TRANS):
            dx = meta[:, 1 + t : 2 + t]
            dy = meta[:, 1 + TRANS + t : 2 + TRANS + t]
            index = (dx + REACH) * SIDE + (dy + REACH)
            picks[t * count : (t + 1) * count] = onehot((spot == index) | (spot == index + COMBOS)).astype(BF16)
            value = -(dx * dx + dy * dy) / (2.0 * offset_sigma * offset_sigma)
            terms.append(jnp.where(lane == 0, value, 0.0))
        coef = square / (2.0 * noise_wide)
        coef = jnp.concatenate([coef] * TRANS, axis=0)
        base = prior - lax.dot_general(power, coef, BY_LANE, precision=HIGH, preferred_element_type=F32)
        base = base + lax.dot_general(
            jnp.ones((owned, LANE), F32), jnp.concatenate(terms, axis=0), BY_LANE,
            precision=HIGH, preferred_element_type=F32,
        )
        calm = 1.0 / noise_wide
        for g in range(GROUPS):
            bright[g] = contrast[:, g * LANE : (g + 1) * LANE]
            quiet[g : g + 1] = calm[:, g * LANE : (g + 1) * LANE]
        return square, base

    def prepare(begin, end):
        @pl.loop(begin // 6, end // 6)
        def _(block):
            for place in range(6):
                tile = block * 6 + place
                phases[tile] = jnp.dot(picks[...], table[tile], preferred_element_type=F32)

    def shifted(tile, g):
        light = bright[g]
        picture = every[:, tile].astype(F32).reshape(count, WIDE)
        real, imag = picture[:, :LANE] * light, picture[:, LANE:] * light
        for t in range(TRANS):
            span = slice(t * count, (t + 1) * count)
            cosine, sine = phases[tile, span, :LANE], phases[tile, span, LANE:]
            yield span, real * cosine - imag * sine, real * sine + imag * cosine

    def build(tile, place, slot, g):
        calm = quiet[pl.ds(g, 1)]
        for span, real, imag in shifted(tile, g):
            slot[span, place * WIDE : place * WIDE + LANE] = (real * calm).astype(BF16)
            slot[span, place * WIDE + LANE : (place + 1) * WIDE] = (imag * calm).astype(BF16)

    loads[8].wait()
    for copy in keeps:
        copy.wait()
    for hop in range(n - 1):
        titles(hop).wait_recv()
    square, base = setup()
    prepare(0, TILES // 2)
    arrive(0)
    prepare(TILES // 2, TILES)

    @pl.loop(0, CHUNKS)
    def _(c):
        @pl.when(c + 1 < CHUNKS)
        def _():
            arrive(c + 1)

        settle(c)
        lefts = []
        for place in range(CHUNK):
            tile = c * CHUNK + place
            build(tile, place, weighted, c)
            lefts.append(turned[c, (COLS - place) * step : (COLS - place) * step + height])
        acc[...] += lax.dot_general(
            jnp.concatenate(lefts, axis=1), weighted[...], BY_LANE, preferred_element_type=F32
        )

    def over_shifts(value, combine):
        total = value
        for t in range(1, TRANS):
            total = combine(total, pltpu.roll(value, t * count, 1))
        return total

    peak = jnp.full((owned, rows), -jnp.inf, F32)
    for r in range(ROT):
        peak = jnp.maximum(peak, acc[r * owned : (r + 1) * owned])
    peak = jnp.max(peak + base, axis=0, keepdims=True)
    peak = over_shifts(jnp.broadcast_to(peak, (8, rows)), jnp.maximum)[:1]
    less = base - peak
    total = jnp.zeros((owned, rows), F32)
    for r in range(ROT):
        expo = jnp.exp(acc[r * owned : (r + 1) * owned] + less)
        acc[r * owned : (r + 1) * owned] = expo
        total = total + expo
    total = jnp.sum(total, axis=0, keepdims=True)
    total = over_shifts(jnp.broadcast_to(total, (8, rows)), jnp.add)[:1]
    stat[0:1] = peak[:, :width]
    stat[1:2] = total[:, :width]

    stats[row_id, column_id] = stat[...]
    pl.semaphore_wait(plane_sem, m - 1)
    slot = stats.at[row_id, column_id]
    shared = [
        send(stat, slot, peer, stat_left.at[k], stat_sem.at[k]) for k, peer in enumerate(others)
    ]

    @pl.loop(0, TILES // 4)
    def _(c):
        for place in range(4):
            tile = c * 4 + place
            for span, real, imag in shifted(tile, lax.div(tile, COLS)):
                inserted[tile, span, :LANE] = real.astype(BF16)
                inserted[tile, span, LANE:] = imag.astype(BF16)

    for copy in shared:
        copy.wait_recv()

    entries = [stats[i, c] for i in range(n) for c in range(m)]
    top = entries[0]
    for entry in entries[1:]:
        top = jnp.maximum(top, entry)
    top = top[:1]
    whole = jnp.zeros((1, width), F32)
    for entry in entries:
        whole = whole + entry[1:2] * jnp.exp(entry[:1] - top)
    logs = jnp.broadcast_to(top + jnp.log(whole), (8, width))
    loglik_ref[...] = pltpu.roll(logs, width - row_id * local, 1)[:1, :local]
    factor = jnp.exp(stat[0:1] - top) / whole
    factor = jnp.concatenate([factor] * (rows // width), axis=1)

    summed = jnp.zeros((owned, rows), F32)
    for r in range(ROT):
        value = (acc[r * owned : (r + 1) * owned] * factor).astype(BF16)
        summed = summed + value.astype(F32)
        shift, q = r // MIX, r % MIX
        for spot in ((COLS - shift) % COLS, (COLS - shift) % COLS + COLS):
            post[spot * step + q * owned : spot * step + (q + 1) * owned] = value
    weight = jnp.sum(summed, axis=1, keepdims=True) * (1.0 / count)
    diagonal = iota((owned, owned), 0) == iota((owned, owned), 1)
    weight_ref[...] = jnp.sum(
        jnp.where(diagonal, jnp.broadcast_to(weight, (owned, owned)), 0.0), axis=0, keepdims=True
    )
    lane = iota((owned, LANE), 1)
    seg = iota((owned, LANE), 1) // SEG
    def insert(g):
        left = jnp.concatenate(
            [post[(COLS - s) * step : (COLS - s) * step + height] for s in range(COLS)], axis=1
        )
        right = jnp.concatenate([inserted[g * COLS + s] for s in range(COLS)], axis=0)
        return jnp.dot(left, right, preferred_element_type=F32)

    def finish(g):
        scale = inverses[g]
        spread_out = [[], []]
        for j in range(COLS):
            halves = []
            for p in range(2):
                half = slice(p * LANE, (p + 1) * LANE)
                value = mixed[j * step : j * step + owned, half]
                for q in range(1, MIX):
                    after = (j + 1) % COLS
                    here = pltpu.roll(mixed[j * step + q * owned : j * step + (q + 1) * owned, half], LANE - q * TURN, 1)
                    there = pltpu.roll(
                        mixed[after * step + q * owned : after * step + (q + 1) * owned, half], LANE - q * TURN, 1
                    )
                    value = value + jnp.where(lane < LANE - q * TURN, here, there)
                halves.append(value * scale)
            value = jnp.concatenate(halves, axis=0)
            high = value.astype(BF16)
            low = (value - high.astype(F32)).astype(BF16)
            value = jnp.dot(jnp.concatenate([high, low], axis=1), unblend[j % LOW], preferred_element_type=F32)
            for p in range(2):
                spread_out[p].append(value[p * owned : (p + 1) * owned])
        for p in range(2):
            for k in range(COLS):
                start = g * SPAN + (p * CYCLES * ANG + k * LANE)
                if not isinstance(g, int):
                    start = pl.multiple_of(start, LANE)
                fresh_ref[:, pl.ds(start, LANE)] = pick_segments(
                    [spread_out[p][(LOW * k + s) % COLS] for s in range(LOW)], seg
                )

    mixed[...] = insert(0)
    denom = jnp.dot(
        over_shifts(summed, jnp.add)[:, :count], square, precision=HIGH, preferred_element_type=F32
    )
    inverse = 1.0 / (denom + tau_wide)
    for g in range(GROUPS):
        inverses[g] = inverse[:, g * LANE : (g + 1) * LANE]

    @pl.loop(1, GROUPS)
    def _(g):
        value = insert(g)
        finish(g - 1)
        mixed[...] = value

    finish(GROUPS - 1)

    for copy in shared + [titles(hop) for hop in range(n - 1)]:
        copy.wait_send()

    @pl.loop(0, CHUNKS)
    def _(c):
        for hop in range(hops):
            outward(c, hop).wait_send()
        for hop in range(hops + 1):
            relay(c, hop).wait_send()


def publish(*refs):
    copies = [pltpu.make_async_copy(refs[k], refs[3 + k], refs[6].at[k]) for k in range(3)]
    for copy in copies:
        copy.start()
    for copy in copies:
        copy.wait()


def per_device(
    images, references, class_logprior, ctf_table, noise_power, tau_power, defocus, offsets
):
    n, m = lax.axis_size("img"), lax.axis_size("cls")
    local = images.shape[0]
    count = local * n
    rows = count * TRANS
    owned_true = references.shape[0]
    owned = -(-owned_true // 16) * 16
    spare = owned - owned_true
    width = max(count, LANE)
    height = ROT * owned
    vmem = pl.BlockSpec(memory_space=pltpu.VMEM)
    hbm = pl.BlockSpec(memory_space=pl.ANY)
    prior = class_logprior
    if spare:
        references = jnp.pad(references, ((0, spare), (0, 0)))
        prior = jnp.pad(class_logprior.astype(F32), (0, spare), constant_values=-1e30)

    dma = pltpu.SemaphoreType.DMA
    hops = n // 2 - 1
    fresh, weight, loglik = pl.pallas_call(
        lambda *refs: kernel(n, m, *refs),
        out_shape=(
            pltpu.VMEM((owned, 2 * CYCLES * ANG), F32),
            pltpu.VMEM((1, owned), F32),
            pltpu.VMEM((1, local), F32),
        ),
        in_specs=[hbm] * 9,
        out_specs=(vmem,) * 3,
        scratch_shapes=[
            pltpu.VMEM((local, 2 * CYCLES * ANG), BF16),
            pltpu.VMEM((owned, 2 * CYCLES * ANG), BF16),
            pltpu.VMEM((1, owned), prior.dtype),
            pltpu.VMEM(ctf_table.shape, F32),
            pltpu.VMEM((1, CYCLES), F32),
            pltpu.VMEM((1, CYCLES), F32),
            pltpu.VMEM((1, local), jnp.int32),
            pltpu.VMEM((TRANS, 2, local), jnp.int32),
            pltpu.VMEM((TILES, TABLE_ROWS, WIDE), BF16),
            pltpu.VMEM((TILES, local, WIDE), BF16),
            pltpu.VMEM((n, TILES, local, WIDE), BF16),
            pltpu.VMEM((COLS, 2 * GROUPS * owned, LANE), F32),
            pltpu.VMEM((LOW, LANE, LANE), BF16),
            pltpu.VMEM((LOW, WIDE, LANE), BF16),
            pltpu.VMEM((GROUPS, 2 * height, WIDE), BF16),
            pltpu.VMEM((rows, CHUNK * WIDE), BF16),
            pltpu.VMEM((TILES, rows, WIDE), BF16),
            pltpu.VMEM((local, LANE), BF16),
            pltpu.VMEM((n, local, LANE), BF16),
            pltpu.VMEM((rows, TABLE_ROWS), BF16),
            pltpu.VMEM((TILES, rows, WIDE), F32),
            pltpu.VMEM((GROUPS, count, LANE), F32),
            pltpu.VMEM((GROUPS, LANE), F32),
            pltpu.VMEM((height, rows), F32),
            pltpu.VMEM((2 * height, rows), BF16),
            pltpu.VMEM((height, WIDE), F32),
            pltpu.VMEM((GROUPS, owned, LANE), F32),
            pltpu.VMEM((2, width), F32),
            pltpu.VMEM((n, m, 2, width), F32),
            dma((9,)),
            dma((CHUNKS, hops)),
            dma((CHUNKS, hops)),
            dma((CHUNKS, hops + 1)),
            dma((CHUNKS, hops + 1)),
            dma((n * m - 1,)),
            dma((n * m - 1,)),
            dma((n - 1,)),
            dma((n - 1,)),
            dma((2,)),
            pltpu.SemaphoreType.REGULAR,
        ],
        compiler_params=pltpu.CompilerParams(
            collective_id=0, has_side_effects=True, vmem_limit_bytes=60 * 1024 * 1024
        ),
        name="classify",
    )(
        images,
        references,
        prior[None],
        ctf_table,
        noise_power[None],
        tau_power[None],
        defocus[None],
        offsets.transpose(1, 2, 0),
        jnp.asarray(phase_rows()),
    )
    shapes = (fresh.shape, weight.shape, loglik.shape)
    fresh, weight, loglik = pl.pallas_call(
        publish,
        out_shape=tuple(jax.ShapeDtypeStruct(shape, F32) for shape in shapes),
        in_specs=[vmem] * 3,
        out_specs=(hbm,) * 3,
        scratch_shapes=[dma((3,))],
        compiler_params=pltpu.CompilerParams(vmem_limit_bytes=1024 * 1024),
        name="publish",
    )(fresh, weight, loglik)
    return fresh[:owned_true], weight[0, :owned_true], loglik[0]


def solution(mesh):
    return jax.shard_map(
        per_device,
        mesh=mesh,
        in_specs=(
            P("img", None),
            P(("img", "cls"), None),
            P(("img", "cls")),
            P(),
            P(),
            P(),
            P("img"),
            P("img", None, None),
        ),
        out_specs=(P(("img", "cls"), None), P(("img", "cls")), P("img")),
        check_vma=False,
    )
```

```python
import math

import jax
import jax.numpy as jnp
import numpy as np
from jax import lax
from jax.experimental import pallas as pl
from jax.experimental.pallas import tpu as pltpu
from jax.sharding import PartitionSpec as P

TRANS = 4
CYCLES = 32
ANG = 144
ROT = 36
NDEF = 16

STRIDE = ANG // ROT
REACH = 3
SIDE = 2 * REACH + 1
COMBOS = SIDE * SIDE
TABLE_ROWS = 112
HIGH = lax.Precision.HIGHEST
offset_sigma = 2.0

LANE = 128
LOW = 8
GROUPS = CYCLES // LOW
SPAN = LOW * ANG
COLS = SPAN // LANE
MIX = ROT // COLS
TURN = LANE // MIX
SEG = LANE // LOW
TILES = GROUPS * COLS
WIDE = 2 * LANE
CHUNK = 9
CHUNKS = TILES // CHUNK
BY_LANE = (((1,), (1,)), ((), ()))
F32 = jnp.float32
BF16 = jnp.bfloat16


def phase_rows():
    group = np.arange(GROUPS)[:, None, None]
    column = np.arange(COLS)[None, :, None]
    lane = np.arange(LANE)[None, None, :]
    radius = group * LOW + lane % LOW + 1.0
    theta = 2.0 * math.pi * (column * SEG + lane // LOW) / ANG
    freq_x = (radius * np.cos(theta)).reshape(TILES, 1, LANE)
    freq_y = (radius * np.sin(theta)).reshape(TILES, 1, LANE)
    combo = np.arange(COMBOS)[None, :, None]
    dx = combo // SIDE - REACH
    dy = combo % SIDE - REACH
    angle = -2.0 * math.pi * (dx * freq_x + dy * freq_y) / (2.0 * CYCLES)
    full = np.concatenate([np.cos(angle), np.sin(angle)], axis=2)
    high = full.astype(jnp.bfloat16)
    low = (full - high.astype(np.float64)).astype(jnp.bfloat16)
    table = np.zeros((TILES, TABLE_ROWS, WIDE), jnp.bfloat16)
    table[:, :COMBOS] = high
    table[:, COMBOS : 2 * COMBOS] = low
    return table


def iota(shape, dim):
    return lax.broadcasted_iota(jnp.int32, shape, dim)


def onehot(mask):
    return jnp.where(mask, 1.0, 0.0).astype(F32)


def column_of(row, size):
    square = jnp.broadcast_to(row, (size, size))
    return jnp.sum(
        jnp.where(iota((size, size), 0) == iota((size, size), 1), square, 0.0), axis=1, keepdims=True
    )


def pick_segments(sources, seg):
    value = sources[0]
    for s in range(1, LOW):
        value = jnp.where(seg == s, sources[s], value)
    return value


def natural_to_mixed(block, j, seg):
    sources = []
    for s in range(LOW):
        cycle = (s - j) % LOW
        n = (cycle * COLS + j - s) // LOW
        sources.append(block(n))
    return pick_segments(sources, seg)


def kernel(
    n, m,
    images_hbm, refs_hbm, prior_hbm, ctf_hbm, noise_hbm, tau_hbm, defocus_hbm, offsets_hbm, table_hbm,
    fresh_ref, weight_ref, loglik_ref,
    images_nat, refs_nat, prior_ref, ctf_ref, noise_ref, tau_ref, defocus_ref, offsets_ref, table, own, every, spin, blend, unblend, turned, weighted, inserted, own_meta, metas, picks, phases, bright, quiet,
    acc, post, mixed, inverses, stat, stats,
    load_sem, left_sem, direct_sem, relay_left, relay_sem, stat_left, stat_sem, meta_left, meta_sem, keep_sem, plane_sem,
):
    local = images_nat.shape[0]
    owned = refs_nat.shape[0]
    count = n * local
    rows = count * TRANS
    width = stat.shape[1]
    height = ROT * owned
    step = MIX * owned

    row_id, column_id = lax.axis_index("img"), lax.axis_index("cls")
    partner = row_id + 1 - 2 * lax.rem(row_id, 2)
    peers = [lax.rem(row_id + 2 * hop, n) for hop in range(1, n // 2)]
    above = [{"cls": lax.rem(column_id + hop, m)} for hop in range(1, m)]
    beside = [{"img": lax.rem(row_id + hop, n)} for hop in range(1, n)]
    others = [
        {"img": lax.rem(row_id + i, n), "cls": lax.rem(column_id + c, m)}
        for c in reversed(range(m)) for i in sorted(range(n), key=lambda i: (i % 2, i), reverse=True) if i or c
    ]

    barrier = pltpu.get_barrier_semaphore()
    for peer in above + beside:
        pl.semaphore_signal(barrier, inc=1, device_id=peer, device_id_type=pl.DeviceIdType.MESH)
    pairs = (
        (images_hbm, images_nat), (defocus_hbm, defocus_ref), (offsets_hbm, offsets_ref), (refs_hbm, refs_nat),
        (prior_hbm, prior_ref), (ctf_hbm, ctf_ref), (noise_hbm, noise_ref), (tau_hbm, tau_ref), (table_hbm, table),
    )
    loads = [pltpu.make_async_copy(src, dst, load_sem.at[k]) for k, (src, dst) in enumerate(pairs)]
    for copy in loads:
        copy.start()

    def send(src, dst, peer, left, landed):
        copy = pltpu.make_async_remote_copy(
            src_ref=src, dst_ref=dst, send_sem=left, recv_sem=landed,
            device_id=peer, device_id_type=pl.DeviceIdType.MESH,
        )
        copy.start()
        return copy

    source = iota((LANE, LANE), 0)
    target = iota((LANE, LANE), 1)
    for j in range(LOW):
        place = (source % SEG) * LOW + (source // SEG + (LOW - j)) % LOW
        blend[j] = onehot(target == place).astype(BF16)
        place = (target % SEG) * LOW + (target // SEG + (LOW - j)) % LOW
        back = onehot(source == place).astype(BF16)
        unblend[j, :LANE] = back
        unblend[j, LANE:] = back

    loads[1].wait()
    loads[2].wait()
    meta = jnp.zeros((local, LANE), F32)
    lane = iota((local, LANE), 1)
    meta = jnp.where(lane == 0, column_of(defocus_ref[...].astype(F32), local), meta)
    for t in range(TRANS):
        for axis in range(2):
            value = column_of(offsets_ref[t, axis : axis + 1].astype(F32), local)
            meta = jnp.where(lane == 1 + t + axis * TRANS, value, meta)
    own_meta[...] = meta.astype(BF16)

    def mix(nat, size, j):
        seg = iota((size, LANE), 1) // SEG
        parts = []
        for g in range(GROUPS):
            for p in range(2):
                start = p * CYCLES * ANG + g * SPAN

                def block(k, start=start):
                    return nat[:, start + k * LANE : start + (k + 1) * LANE].astype(F32)

                parts.append(natural_to_mixed(block, j, seg))
        stacked = jnp.concatenate(parts, axis=0).astype(BF16)
        return jnp.dot(stacked, blend[j % LOW], preferred_element_type=F32)

    loads[0].wait()
    for j in range(COLS):
        moved = mix(images_nat, local, j).astype(BF16)
        for g in range(GROUPS):
            for p in range(2):
                index = g * 2 + p
                own[g * COLS + j, :, p * LANE : (p + 1) * LANE] = moved[
                    index * local : (index + 1) * local
                ]

    pl.semaphore_wait(barrier, n + m - 2)
    for peer in above:
        pl.semaphore_signal(plane_sem, inc=1, device_id=peer, device_id_type=pl.DeviceIdType.MESH)

    def remote(src, dst, peer, left, landed):
        return pltpu.make_async_remote_copy(
            src_ref=src, dst_ref=dst, send_sem=left, recv_sem=landed,
            device_id=peer, device_id_type=pl.DeviceIdType.MESH,
        )

    def outward(c, hop):
        piece = pl.ds(c * CHUNK, CHUNK)
        return remote(
            own.at[piece], every.at[row_id, piece], {"img": peers[hop]}, left_sem.at[c, hop], direct_sem.at[c, hop]
        )

    def relay(c, hop):
        piece = pl.ds(c * CHUNK, CHUNK)
        if hop == 0:
            src, dst = own.at[piece], every.at[row_id, piece]
        else:
            src = dst = every.at[lax.rem(row_id + n - 2 * hop, n), piece]
        return remote(src, dst, {"img": partner}, relay_left.at[c, hop], relay_sem.at[c, hop])

    def titles(hop):
        return remote(own_meta, metas.at[row_id], beside[hop], meta_left.at[hop], meta_sem.at[hop])

    hops = len(peers)
    for hop in range(n - 1):
        titles(hop).start()
    for c in range(CHUNKS):
        for hop in range(hops):
            outward(c, hop).start()
        relay(c, 0).start()
    keeps = [
        pltpu.make_async_copy(own, every.at[row_id], keep_sem.at[0]),
        pltpu.make_async_copy(own_meta, metas.at[row_id], keep_sem.at[1]),
    ]
    for copy in keeps:
        copy.start()
    acc[...] = jnp.zeros(acc.shape, F32)
    loads[3].wait()
    for j in range(COLS):
        spin[j] = mix(refs_nat, owned, j)
    lane = iota((2 * GROUPS * owned, LANE), 1)
    for q in range(MIX):
        before = pltpu.roll(spin[COLS - 1], q * TURN, 1) if q else None
        for j in range(COLS):
            if q:
                here = pltpu.roll(spin[j], q * TURN, 1)
                value = jnp.where(lane < q * TURN, before, here).astype(BF16)
                before = here
            else:
                value = spin[j].astype(BF16)
            for g in range(GROUPS):
                for p in range(2):
                    index = g * 2 + p
                    for spot in ((COLS - j) % COLS, (COLS - j) % COLS + COLS):
                        turned[
                            g, spot * step + q * owned : spot * step + (q + 1) * owned, p * LANE : (p + 1) * LANE
                        ] = value[index * owned : (index + 1) * owned]
    power = [jnp.zeros((owned, LANE), F32) for _ in range(GROUPS)]
    for j in range(COLS):
        for g in range(GROUPS):
            for p in range(2):
                index = g * 2 + p
                entry = spin[j, index * owned : (index + 1) * owned]
                power[g] = power[g] + entry * entry
    power = jnp.concatenate(power, axis=1)
    spread = onehot(
        iota((CYCLES, GROUPS * LANE), 0)
        == iota((CYCLES, GROUPS * LANE), 1) // LANE * LOW + iota((CYCLES, GROUPS * LANE), 1) % LOW
    )

    def widen(value):
        return jnp.dot(value, spread, precision=HIGH, preferred_element_type=F32)

    for copy in loads[4:8]:
        copy.wait()
    ctf_wide = widen(ctf_ref[...])
    noise_wide = widen(jnp.broadcast_to(noise_ref[...], (8, CYCLES)))[:1]
    tau_wide = widen(jnp.broadcast_to(1.0 / tau_ref[...], (8, CYCLES)))[:1]
    prior = column_of(prior_ref[...].astype(F32), owned)

    def arrive(c):
        for hop in range(hops):
            outward(c, hop).wait_recv()
            relay(c, hop + 1).start()

    def settle(c):
        for hop in range(hops + 1):
            relay(c, hop).wait_recv()

    def setup():
        meta = metas[...].astype(F32).reshape(count, LANE)
        group = iota((count, NDEF), 1).astype(F32)
        chosen = onehot(group == meta[:, :1])
        contrast = jnp.dot(chosen, ctf_wide, precision=HIGH, preferred_element_type=F32)
        square = contrast * contrast
        spot = iota((count, TABLE_ROWS), 1).astype(F32)
        lane = iota((count, LANE), 1)
        terms = []
        for t in range(TRANS):
            dx = meta[:, 1 + t : 2 + t]
            dy = meta[:, 1 + TRANS + t : 2 + TRANS + t]
            index = (dx + REACH) * SIDE + (dy + REACH)
            picks[t * count : (t + 1) * count] = onehot((spot == index) | (spot == index + COMBOS)).astype(BF16)
            value = -(dx * dx + dy * dy) / (2.0 * offset_sigma * offset_sigma)
            terms.append(jnp.where(lane == 0, value, 0.0))
        coef = square / (2.0 * noise_wide)
        coef = jnp.concatenate([coef] * TRANS, axis=0)
        base = prior - lax.dot_general(power, coef, BY_LANE, precision=HIGH, preferred_element_type=F32)
        base = base + lax.dot_general(
            jnp.ones((owned, LANE), F32), jnp.concatenate(terms, axis=0), BY_LANE,
            precision=HIGH, preferred_element_type=F32,
        )
        calm = 1.0 / noise_wide
        for g in range(GROUPS):
            bright[g] = contrast[:, g * LANE : (g + 1) * LANE]
            quiet[g : g + 1] = calm[:, g * LANE : (g + 1) * LANE]
        return square, base

    def prepare(begin, end):
        @pl.loop(begin // 6, end // 6)
        def _(block):
            for place in range(6):
                tile = block * 6 + place
                phases[tile] = jnp.dot(picks[...], table[tile], preferred_element_type=F32)

    def shifted(tile, g):
        light = bright[g]
        picture = every[:, tile].astype(F32).reshape(count, WIDE)
        real, imag = picture[:, :LANE] * light, picture[:, LANE:] * light
        for t in range(TRANS):
            span = slice(t * count, (t + 1) * count)
            cosine, sine = phases[tile, span, :LANE], phases[tile, span, LANE:]
            yield span, real * cosine - imag * sine, real * sine + imag * cosine

    def build(tile, place, slot, g):
        calm = quiet[pl.ds(g, 1)]
        for span, real, imag in shifted(tile, g):
            slot[span, place * WIDE : place * WIDE + LANE] = (real * calm).astype(BF16)
            slot[span, place * WIDE + LANE : (place + 1) * WIDE] = (imag * calm).astype(BF16)

    loads[8].wait()
    for copy in keeps:
        copy.wait()
    for hop in range(n - 1):
        titles(hop).wait_recv()
    square, base = setup()
    prepare(0, TILES // 2)
    arrive(0)
    prepare(TILES // 2, TILES)

    @pl.loop(0, CHUNKS)
    def _(c):
        @pl.when(c + 1 < CHUNKS)
        def _():
            arrive(c + 1)

        settle(c)
        lefts = []
        for place in range(CHUNK):
            tile = c * CHUNK + place
            build(tile, place, weighted, c)
            lefts.append(turned[c, (COLS - place) * step : (COLS - place) * step + height])
        acc[...] += lax.dot_general(
            jnp.concatenate(lefts, axis=1), weighted[...], BY_LANE, preferred_element_type=F32
        )

    def over_shifts(value, combine):
        total = value
        for t in range(1, TRANS):
            total = combine(total, pltpu.roll(value, t * count, 1))
        return total

    peak = jnp.full((owned, rows), -jnp.inf, F32)
    for r in range(ROT):
        peak = jnp.maximum(peak, acc[r * owned : (r + 1) * owned])
    peak = jnp.max(peak + base, axis=0, keepdims=True)
    peak = over_shifts(jnp.broadcast_to(peak, (8, rows)), jnp.maximum)[:1]
    less = base - peak
    total = jnp.zeros((owned, rows), F32)
    for r in range(ROT):
        expo = jnp.exp(acc[r * owned : (r + 1) * owned] + less)
        acc[r * owned : (r + 1) * owned] = expo
        total = total + expo
    total = jnp.sum(total, axis=0, keepdims=True)
    total = over_shifts(jnp.broadcast_to(total, (8, rows)), jnp.add)[:1]
    stat[0:1] = peak[:, :width]
    stat[1:2] = total[:, :width]

    stats[row_id, column_id] = stat[...]
    pl.semaphore_wait(plane_sem, m - 1)
    slot = stats.at[row_id, column_id]
    shared = [
        send(stat, slot, peer, stat_left.at[k], stat_sem.at[k]) for k, peer in enumerate(others)
    ]

    @pl.loop(0, TILES // 4)
    def _(c):
        for place in range(4):
            tile = c * 4 + place
            for span, real, imag in shifted(tile, lax.div(tile, COLS)):
                inserted[tile, span, :LANE] = real.astype(BF16)
                inserted[tile, span, LANE:] = imag.astype(BF16)

    for copy in shared:
        copy.wait_recv()

    entries = [stats[i, c] for i in range(n) for c in range(m)]
    top = entries[0]
    for entry in entries[1:]:
        top = jnp.maximum(top, entry)
    top = top[:1]
    whole = jnp.zeros((1, width), F32)
    for entry in entries:
        whole = whole + entry[1:2] * jnp.exp(entry[:1] - top)
    logs = jnp.broadcast_to(top + jnp.log(whole), (8, width))
    loglik_ref[...] = pltpu.roll(logs, width - row_id * local, 1)[:1, :local]
    factor = jnp.exp(stat[0:1] - top) / whole
    factor = jnp.concatenate([factor] * (rows // width), axis=1)

    summed = jnp.zeros((owned, rows), F32)
    for r in range(ROT):
        value = (acc[r * owned : (r + 1) * owned] * factor).astype(BF16)
        summed = summed + value.astype(F32)
        shift, q = r // MIX, r % MIX
        for spot in ((COLS - shift) % COLS, (COLS - shift) % COLS + COLS):
            post[spot * step + q * owned : spot * step + (q + 1) * owned] = value
    weight = jnp.sum(summed, axis=1, keepdims=True) * (1.0 / count)
    diagonal = iota((owned, owned), 0) == iota((owned, owned), 1)
    weight_ref[...] = jnp.sum(
        jnp.where(diagonal, jnp.broadcast_to(weight, (owned, owned)), 0.0), axis=0, keepdims=True
    )
    lane = iota((owned, LANE), 1)
    seg = iota((owned, LANE), 1) // SEG
    def insert(g):
        left = jnp.concatenate(
            [post[(COLS - s) * step : (COLS - s) * step + height] for s in range(COLS)], axis=1
        )
        right = jnp.concatenate([inserted[g * COLS + s] for s in range(COLS)], axis=0)
        return jnp.dot(left, right, preferred_element_type=F32)

    def finish(g):
        scale = inverses[g]
        spread_out = [[], []]
        for j in range(COLS):
            halves = []
            for p in range(2):
                half = slice(p * LANE, (p + 1) * LANE)
                value = mixed[j * step : j * step + owned, half]
                for q in range(1, MIX):
                    after = (j + 1) % COLS
                    here = pltpu.roll(mixed[j * step + q * owned : j * step + (q + 1) * owned, half], LANE - q * TURN, 1)
                    there = pltpu.roll(
                        mixed[after * step + q * owned : after * step + (q + 1) * owned, half], LANE - q * TURN, 1
                    )
                    value = value + jnp.where(lane < LANE - q * TURN, here, there)
                halves.append(value * scale)
            value = jnp.concatenate(halves, axis=0)
            high = value.astype(BF16)
            low = (value - high.astype(F32)).astype(BF16)
            value = jnp.dot(jnp.concatenate([high, low], axis=1), unblend[j % LOW], preferred_element_type=F32)
            for p in range(2):
                spread_out[p].append(value[p * owned : (p + 1) * owned])
        for p in range(2):
            for k in range(COLS):
                start = g * SPAN + (p * CYCLES * ANG + k * LANE)
                if not isinstance(g, int):
                    start = pl.multiple_of(start, LANE)
                fresh_ref[:, pl.ds(start, LANE)] = pick_segments(
                    [spread_out[p][(LOW * k + s) % COLS] for s in range(LOW)], seg
                )

    mixed[...] = insert(0)
    denom = jnp.dot(
        over_shifts(summed, jnp.add)[:, :count], square, precision=HIGH, preferred_element_type=F32
    )
    inverse = 1.0 / (denom + tau_wide)
    for g in range(GROUPS):
        inverses[g] = inverse[:, g * LANE : (g + 1) * LANE]

    @pl.loop(1, GROUPS)
    def _(g):
        value = insert(g)
        finish(g - 1)
        mixed[...] = value

    finish(GROUPS - 1)

    for copy in shared + [titles(hop) for hop in range(n - 1)]:
        copy.wait_send()

    @pl.loop(0, CHUNKS)
    def _(c):
        for hop in range(hops):
            outward(c, hop).wait_send()
        for hop in range(hops + 1):
            relay(c, hop).wait_send()


def publish(*refs):
    copies = [pltpu.make_async_copy(refs[k], refs[3 + k], refs[6].at[k]) for k in range(3)]
    for copy in copies:
        copy.start()
    for copy in copies:
        copy.wait()


def per_device(
    images, references, class_logprior, ctf_table, noise_power, tau_power, defocus, offsets
):
    n, m = lax.axis_size("img"), lax.axis_size("cls")
    local = images.shape[0]
    count = local * n
    rows = count * TRANS
    owned_true = references.shape[0]
    owned = -(-owned_true // 16) * 16
    spare = owned - owned_true
    width = max(count, LANE)
    height = ROT * owned
    vmem = pl.BlockSpec(memory_space=pltpu.VMEM)
    hbm = pl.BlockSpec(memory_space=pl.ANY)
    prior = class_logprior
    if spare:
        references = jnp.pad(references, ((0, spare), (0, 0)))
        prior = jnp.pad(class_logprior.astype(F32), (0, spare), constant_values=-1e30)

    dma = pltpu.SemaphoreType.DMA
    hops = n // 2 - 1
    fresh, weight, loglik = pl.pallas_call(
        lambda *refs: kernel(n, m, *refs),
        out_shape=(
            pltpu.VMEM((owned, 2 * CYCLES * ANG), F32),
            pltpu.VMEM((1, owned), F32),
            pltpu.VMEM((1, local), F32),
        ),
        in_specs=[hbm] * 9,
        out_specs=(vmem,) * 3,
        scratch_shapes=[
            pltpu.VMEM((local, 2 * CYCLES * ANG), BF16),
            pltpu.VMEM((owned, 2 * CYCLES * ANG), BF16),
            pltpu.VMEM((1, owned), prior.dtype),
            pltpu.VMEM(ctf_table.shape, F32),
            pltpu.VMEM((1, CYCLES), F32),
            pltpu.VMEM((1, CYCLES), F32),
            pltpu.VMEM((1, local), jnp.int32),
            pltpu.VMEM((TRANS, 2, local), jnp.int32),
            pltpu.VMEM((TILES, TABLE_ROWS, WIDE), BF16),
            pltpu.VMEM((TILES, local, WIDE), BF16),
            pltpu.VMEM((n, TILES, local, WIDE), BF16),
            pltpu.VMEM((COLS, 2 * GROUPS * owned, LANE), F32),
            pltpu.VMEM((LOW, LANE, LANE), BF16),
            pltpu.VMEM((LOW, WIDE, LANE), BF16),
            pltpu.VMEM((GROUPS, 2 * height, WIDE), BF16),
            pltpu.VMEM((rows, CHUNK * WIDE), BF16),
            pltpu.VMEM((TILES, rows, WIDE), BF16),
            pltpu.VMEM((local, LANE), BF16),
            pltpu.VMEM((n, local, LANE), BF16),
            pltpu.VMEM((rows, TABLE_ROWS), BF16),
            pltpu.VMEM((TILES, rows, WIDE), F32),
            pltpu.VMEM((GROUPS, count, LANE), F32),
            pltpu.VMEM((GROUPS, LANE), F32),
            pltpu.VMEM((height, rows), F32),
            pltpu.VMEM((2 * height, rows), BF16),
            pltpu.VMEM((height, WIDE), F32),
            pltpu.VMEM((GROUPS, owned, LANE), F32),
            pltpu.VMEM((2, width), F32),
            pltpu.VMEM((n, m, 2, width), F32),
            dma((9,)),
            dma((CHUNKS, hops)),
            dma((CHUNKS, hops)),
            dma((CHUNKS, hops + 1)),
            dma((CHUNKS, hops + 1)),
            dma((n * m - 1,)),
            dma((n * m - 1,)),
            dma((n - 1,)),
            dma((n - 1,)),
            dma((2,)),
            pltpu.SemaphoreType.REGULAR,
        ],
        compiler_params=pltpu.CompilerParams(
            collective_id=0, has_side_effects=True, vmem_limit_bytes=60 * 1024 * 1024
        ),
        name="classify",
    )(
        images,
        references,
        prior[None],
        ctf_table,
        noise_power[None],
        tau_power[None],
        defocus[None],
        offsets.transpose(1, 2, 0),
        jnp.asarray(phase_rows()),
    )
    shapes = (fresh.shape, weight.shape, loglik.shape)
    fresh, weight, loglik = pl.pallas_call(
        publish,
        out_shape=tuple(jax.ShapeDtypeStruct(shape, F32) for shape in shapes),
        in_specs=[vmem] * 3,
        out_specs=(hbm,) * 3,
        scratch_shapes=[dma((3,))],
        compiler_params=pltpu.CompilerParams(vmem_limit_bytes=1024 * 1024),
        name="publish",
    )(fresh, weight, loglik)
    return fresh[:owned_true], weight[0, :owned_true], loglik[0]


def solution(mesh):
    return jax.shard_map(
        per_device,
        mesh=mesh,
        in_specs=(
            P("img", None),
            P(("img", "cls"), None),
            P(("img", "cls")),
            P(),
            P(),
            P(),
            P("img"),
            P("img", None, None),
        ),
        out_specs=(P(("img", "cls"), None), P(("img", "cls")), P("img")),
        check_vma=False,
    )
```
